16 devices in a mesh: batch: 2 (over y, z), time: 8 (over x, core).
Axes of the slice: x: 4, y: 2, z: 1, core: 2. Of those that a mesh axis runs over, the one named last changes fastest.
The devices are a block of a 4x4x8 slice.
Arguments:
- latent: bfloat16 [768, 4, 48, 128], P(('batch', 'time')), parts along dimension 0
- conv_w: bfloat16 [4, 3, 3, 3, 128, 128], replicated
- conv_b: float32 [4, 128], replicated
- norm_g: float32 [5, 128], replicated
- norm_b: float32 [5, 128], replicated
- attn_w: bfloat16 [4, 128, 128], replicated
- attn_b: float32 [4, 128], replicated
Outputs:
- output: bfloat16 [768, 4, 48, 128], P(('batch', 'time')), parts along dimension 0
There are 2 independent parts. The reference program is written for one: setup_inputs(seed, part) draws one part's arguments, and reference() takes and returns one part's arrays. A program takes and returns all parts, laid end to end along the dimension named above; an argument that names none is the same for every part.
All inputs are finite; a program needn't handle non-finite values.
Results may differ from the reference program's by a relative error of at most 0.0139455.
Values are sent between devices in bfloat16 or wider.
A program may use at most 768 MiB of HBM per device.

```python
import jax
import jax.numpy as jnp
from jax import lax

FRAMES = 384
HEIGHT = 4
WIDTH = 48
CHANNELS = 128
GROUPS = 32
NORM_EPS = 1e-6


def setup_inputs(seed: int = 0, part: int = 0) -> dict:
    part_key = jax.random.fold_in(jax.random.key(seed), part)
    video_keys = jax.random.split(part_key, 4)
    weight_keys = jax.random.split(jax.random.key(seed + 1), 6)
    time_pos = jnp.arange(FRAMES, dtype=jnp.float32) / max(FRAMES - 1, 1) - 0.5
    time_slope = 1.4 + 0.4 * jax.random.uniform(video_keys[0], (), jnp.float32)
    frame_scale = jnp.exp(time_slope * time_pos)[:, None, None, None]
    chan_offset = jax.random.normal(video_keys[1], (CHANNELS,), jnp.float32)
    frame_mean = time_pos[:, None, None, None] * chan_offset
    shared_noise = jax.random.normal(video_keys[2], (1, HEIGHT, WIDTH, CHANNELS), jnp.float32)
    fresh_noise = jax.random.normal(video_keys[3], (FRAMES, HEIGHT, WIDTH, CHANNELS), jnp.float32)
    latent = frame_scale * (0.5 * shared_noise + 0.85 * fresh_noise) + frame_mean
    conv_w = jax.random.normal(weight_keys[0], (4, 3, 3, 3, CHANNELS, CHANNELS), jnp.float32) * (27 * CHANNELS) ** -0.5
    conv_b = 0.3 * jax.random.normal(weight_keys[1], (4, CHANNELS), jnp.float32)
    norm_g = 1.0 + 0.3 * jax.random.normal(weight_keys[2], (5, CHANNELS), jnp.float32)
    norm_b = 0.3 * jax.random.normal(weight_keys[3], (5, CHANNELS), jnp.float32)
    attn_w = jax.random.normal(weight_keys[4], (4, CHANNELS, CHANNELS), jnp.float32) * CHANNELS ** -0.5
    attn_b = 0.3 * jax.random.normal(weight_keys[5], (4, CHANNELS), jnp.float32)
    return {"latent": latent.astype(jnp.bfloat16), "conv_w": conv_w.astype(jnp.bfloat16), "conv_b": conv_b, "norm_g": norm_g, "norm_b": norm_b, "attn_w": attn_w.astype(jnp.bfloat16), "attn_b": attn_b}


def group_norm(feature, norm_gain, norm_shift):
    values_f = feature.astype(jnp.float32)
    grouped = values_f.reshape(FRAMES, HEIGHT, WIDTH, GROUPS, CHANNELS // GROUPS)
    elem_count = FRAMES * HEIGHT * WIDTH * (CHANNELS // GROUPS)
    group_mean = jnp.sum(grouped, axis=(0, 1, 2, 4)) / elem_count
    group_sq = jnp.sum(grouped * grouped, axis=(0, 1, 2, 4)) / elem_count
    inv_std = lax.rsqrt(group_sq - group_mean * group_mean + NORM_EPS)
    mean_full = jnp.repeat(group_mean, CHANNELS // GROUPS)
    scale_full = jnp.repeat(inv_std, CHANNELS // GROUPS) * norm_gain
    return (values_f - mean_full) * scale_full + norm_shift


def causal_conv(activation, kernel, conv_bias):
    padded = jnp.concatenate([activation[:1], activation[:1], activation], axis=0)
    conv_out = lax.conv_general_dilated(padded[None].astype(jnp.float32), kernel.astype(jnp.float32), (1, 1, 1), ((0, 0), (1, 1), (1, 1)), dimension_numbers=("NDHWC", "DHWIO", "NDHWC"))
    return (conv_out[0] + conv_bias).astype(jnp.bfloat16)


def resnet_block(feature, conv_w, conv_b, norm_g, norm_b, norm_first, conv_first):
    activation = jax.nn.silu(group_norm(feature, norm_g[norm_first], norm_b[norm_first])).astype(jnp.bfloat16)
    branch = causal_conv(activation, conv_w[conv_first], conv_b[conv_first])
    activation = jax.nn.silu(group_norm(branch, norm_g[norm_first + 1], norm_b[norm_first + 1])).astype(jnp.bfloat16)
    branch = causal_conv(activation, conv_w[conv_first + 1], conv_b[conv_first + 1])
    return (feature.astype(jnp.float32) + branch.astype(jnp.float32)).astype(jnp.bfloat16)


def spatial_attention(feature, norm_gain, norm_shift, attn_w, attn_b):
    normed = group_norm(feature, norm_gain, norm_shift).astype(jnp.bfloat16)
    tokens = normed.reshape(FRAMES, HEIGHT * WIDTH, CHANNELS)
    score_scale = CHANNELS ** -0.5

    def one_frame(frame_tok):
        queries = (jnp.dot(frame_tok, attn_w[0], preferred_element_type=jnp.float32) + attn_b[0]).astype(jnp.bfloat16)
        keys_t = (jnp.dot(frame_tok, attn_w[1], preferred_element_type=jnp.float32) + attn_b[1]).astype(jnp.bfloat16)
        values_t = (jnp.dot(frame_tok, attn_w[2], preferred_element_type=jnp.float32) + attn_b[2]).astype(jnp.bfloat16)
        scores = jnp.dot(queries, keys_t.T, preferred_element_type=jnp.float32) * score_scale
        attn_probs = jax.nn.softmax(scores, axis=-1).astype(jnp.bfloat16)
        mixed_val = jnp.dot(attn_probs, values_t, preferred_element_type=jnp.float32).astype(jnp.bfloat16)
        return (jnp.dot(mixed_val, attn_w[3], preferred_element_type=jnp.float32) + attn_b[3]).astype(jnp.bfloat16)

    projected = lax.map(one_frame, tokens).reshape(feature.shape)
    return (feature.astype(jnp.float32) + projected.astype(jnp.float32)).astype(jnp.bfloat16)


def reference(latent, conv_w, conv_b, norm_g, norm_b, attn_w, attn_b):
    feature = resnet_block(latent, conv_w, conv_b, norm_g, norm_b, 0, 0)
    feature = spatial_attention(feature, norm_g[2], norm_b[2], attn_w, attn_b)
    return resnet_block(feature, conv_w, conv_b, norm_g, norm_b, 3, 2)
```

```python
import functools

import jax
import jax.numpy as jnp
from jax import lax
from jax.experimental import pallas as pl
from jax.experimental.pallas import tpu as pltpu
from jax.sharding import PartitionSpec as P

GROUPS = 32
NORM_EPS = 1e-6
TILE = 8
ATT = 2
CHUNKS = 4
HALO = 2
MESH_ID = pl.DeviceIdType.MESH
F32, BF16 = jnp.float32, jnp.bfloat16


def dot(a, b):
    return jnp.dot(a, b, preferred_element_type=F32)


def vreg_sum(value):
    return jnp.sum(value.reshape(-1, 8, value.shape[-1]), axis=0)


def kernel(n_dev, latent, conv_w, conv_b, norm_g, norm_b, attn_w, attn_b, out, x_ref, h_ref, ua, ub, w_ref, aw_ref, cb_ref, g_ref, b_ref, ab_ref, halo, stats, in_sem, par_sem, out_sem, halo_send, halo_recv, stat_send, stat_recv):
    frames, height, width, chan = latent.shape
    me = lax.axis_index("time")
    tiles = frames // TILE
    piece = frames // CHUNKS
    elem_count = n_dev * frames * height * width * (chan // GROUPS)

    in_copies = [pltpu.make_async_copy(latent.at[pl.ds(c * piece, piece)], x_ref.at[pl.ds(HALO + c * piece, piece)], in_sem.at[c]) for c in range(CHUNKS)]
    for c in reversed(range(CHUNKS)):
        in_copies[c].start()
    pairs = [(norm_g, g_ref), (norm_b, b_ref), (conv_b, cb_ref), (attn_w, aw_ref), (attn_b, ab_ref), (conv_w, w_ref)]
    par_copies = [pltpu.make_async_copy(src, dst, par_sem.at[i]) for i, (src, dst) in enumerate(pairs)]
    for copy in par_copies:
        copy.start()

    barrier = pltpu.get_barrier_semaphore()
    for k in range(1, n_dev):
        pl.semaphore_signal(barrier, inc=1, device_id={"time": lax.rem(me + k, n_dev)}, device_id_type=MESH_ID)
    pl.semaphore_wait(barrier, n_dev - 1)

    def halo_copy(slot, src, start):
        return pltpu.make_async_remote_copy(src_ref=src.at[pl.ds(start, HALO)], dst_ref=halo.at[slot], send_sem=halo_send.at[slot], recv_sem=halo_recv.at[slot], device_id={"time": lax.rem(me + 1, n_dev)}, device_id_type=MESH_ID)

    def send_halo(slot, src):
        @pl.when(me < n_dev - 1)
        def _():
            halo_copy(slot, src, frames).start()

    def take_halo(slot, src):
        @pl.when(me > 0)
        def _():
            halo_copy(slot, src, frames).wait_recv()
            src[pl.ds(0, HALO)] = halo[slot]

        @pl.when(me == 0)
        def _():
            for f in range(HALO):
                src[f] = src[HALO]

        @pl.when(me < n_dev - 1)
        def _():
            halo_copy(slot, src, frames).wait_send()

    lane = lax.broadcasted_iota(jnp.int32, (8, chan), 1)

    def exchange(stage, sums):
        both = jnp.concatenate([jnp.sum(sums[0], axis=0, keepdims=True), jnp.sum(sums[1], axis=0, keepdims=True), jnp.zeros((6, chan), F32)], axis=0)
        stats[stage, me] = both

        def copy_to(k):
            return pltpu.make_async_remote_copy(src_ref=stats.at[stage, me], dst_ref=stats.at[stage, me], send_sem=stat_send.at[stage, k], recv_sem=stat_recv.at[stage, n_dev - k], device_id={"time": lax.rem(me + k, n_dev)}, device_id_type=MESH_ID)

        def copy_from(k):
            peer = lax.rem(me + k, n_dev)
            return pltpu.make_async_remote_copy(src_ref=stats.at[stage, peer], dst_ref=stats.at[stage, peer], send_sem=stat_send.at[stage, k], recv_sem=stat_recv.at[stage, k], device_id={"time": peer}, device_id_type=MESH_ID)

        for k in range(1, n_dev):
            copy_to(k).start()
        for k in range(1, n_dev):
            copy_from(k).wait_recv()
        total = stats[stage, 0]
        for d in range(1, n_dev):
            total = total + stats[stage, d]
        for k in range(1, n_dev):
            copy_to(k).wait_send()
        per_group = chan // GROUPS
        step = 1
        while step < per_group:
            swap = jnp.where(lax.rem(lane, 2 * step) < step, pltpu.roll(total, chan - step, 1), pltpu.roll(total, step, 1))
            total = total + swap
            step *= 2
        mean = total[0:1] / elem_count
        inv_std = lax.rsqrt(total[1:2] / elem_count - mean * mean + NORM_EPS)
        return mean, inv_std * g_ref[pl.ds(stage, 1)], b_ref[pl.ds(stage, 1)]

    col = lax.rem(lax.broadcasted_iota(jnp.int32, (height * width, chan), 0), width)

    def norm_tile(src, dst, tile, coef):
        mean, scale, shift = coef
        for f in range(TILE + HALO):
            value = src[tile * TILE + f].astype(F32).reshape(height * width, chan)
            half = 0.5 * ((value - mean) * scale + shift)
            act = half + half * jnp.tanh(half)
            left = jnp.where(col == 0, 0.0, pltpu.roll(act, 1, 0))
            right = jnp.where(col == width - 1, 0.0, pltpu.roll(act, height * width - 1, 0))
            for e, moved in enumerate((left, act, right)):
                dst[:, f, :, e * chan:(e + 1) * chan] = moved.astype(BF16).reshape(height, width, chan)

    zero_w = jnp.zeros((chan, chan), BF16)

    def conv_tile(u, k, bias):
        def cols(row, first, count, e):
            return u[row, first:first + count, :, e * chan:(e + 1) * chan].reshape(count * width, chan)

        lhs, rhs = [], []
        for a in range(3):
            for e in range(3):
                for side in range(2):
                    lhs.append(jnp.concatenate([cols(g + side, a, TILE, e) for g in range(0, height, 2)], axis=0))
                    rhs.append(jnp.concatenate([w_ref[k, a, 1 + side, e], w_ref[k, a, side, e]], axis=1))
        main = dot(jnp.concatenate(lhs, axis=1), jnp.concatenate(rhs, axis=0))

        def extra(row, d):
            lhs, rhs = [], []
            for s in range(4):
                for e in range(3):
                    lhs.append(jnp.concatenate([cols(row, 2 * p + s, 1, e) for p in range(TILE // 2)], axis=0))
                    rhs.append(jnp.concatenate([w_ref[k, s, d, e] if s < 3 else zero_w, w_ref[k, s - 1, d, e] if s > 0 else zero_w], axis=1))
            return dot(jnp.concatenate(lhs, axis=1), jnp.concatenate(rhs, axis=0))

        lower = extra(2, 2)
        upper = extra(1, 0)
        rows = []
        for f in range(TILE):
            here = slice(f * width, (f + 1) * width)
            there = slice((TILE + f) * width, (TILE + f + 1) * width)
            pair = slice((f // 2) * width, (f // 2 + 1) * width)
            half = slice((f % 2) * chan, (f % 2 + 1) * chan)
            rows.append([main[here, :chan] + bias, main[here, chan:] + lower[pair, half] + bias, main[there, :chan] + upper[pair, half] + bias, main[there, chan:] + bias])
        return rows

    def conv_stage(k, src, coef, emit, after):
        bias = cb_ref[pl.ds(k, 1)]
        norm_tile(src, ua, tiles - 1, coef)

        def finish(u, tile, sums):
            rows = conv_tile(u, k, bias)
            for f in range(TILE):
                for i in range(height):
                    value = emit(tile * TILE + f, i, rows[f][i].astype(BF16)).astype(F32)
                    sums = (sums[0] + vreg_sum(value), sums[1] + vreg_sum(value * value))
            return sums

        def body(it, sums):
            high = tiles - 1 - 2 * it
            norm_tile(src, ub, high - 1, coef)
            sums = finish(ua, high, sums)
            norm_tile(src, ua, jnp.maximum(high - 2, 0), coef)
            sums = finish(ub, high - 1, sums)
            after(it, high)
            return sums

        zero = jnp.zeros((8, chan), F32)
        return lax.fori_loop(0, tiles // 2, body, (zero, zero))

    def into_h(frame, i, value):
        h_ref[HALO + frame, i] = value
        return value

    def into_x(frame, i, value):
        value = (x_ref[HALO + frame, i].astype(F32) + value.astype(F32)).astype(BF16)
        x_ref[HALO + frame, i] = value
        return value

    def send_first(slot, src):
        def after(it, high):
            @pl.when(it == 0)
            def _():
                send_halo(slot, src)
        return after

    def nothing(it, high):
        pass

    def out_copy(it):
        first = frames - 2 * TILE * (it + 1)
        return pltpu.make_async_copy(x_ref.at[pl.ds(HALO + first, 2 * TILE)], out.at[pl.ds(first, 2 * TILE)], out_sem.at[it])

    def write_out(it, high):
        out_copy(it).start()

    zero = jnp.zeros((8, chan), F32)
    sums = (zero, zero)
    for c in reversed(range(CHUNKS)):
        in_copies[c].wait()
        if c == CHUNKS - 1:
            send_halo(0, x_ref)

        def add_frame(f, sums):
            value = x_ref[HALO + c * piece + f].astype(F32)
            return sums[0] + vreg_sum(value), sums[1] + vreg_sum(value * value)

        sums = lax.fori_loop(0, piece, add_frame, sums)
    for copy in par_copies:
        copy.wait()

    coef = exchange(0, sums)
    take_halo(0, x_ref)
    sums = conv_stage(0, x_ref, coef, into_h, send_first(1, h_ref))
    coef = exchange(1, sums)
    take_halo(1, h_ref)
    sums = conv_stage(1, h_ref, coef, into_x, nothing)
    mean, scale, shift = exchange(2, sums)

    tokens = height * width
    qkv_w = jnp.concatenate([aw_ref[0], aw_ref[1], aw_ref[2]], axis=1)
    qkv_b = jnp.concatenate([ab_ref[0:1], ab_ref[1:2], ab_ref[2:3]], axis=1)
    out_b = ab_ref[3:4]
    gain = chan ** -0.5 * 1.4426950408889634

    def attend(it, sums):
        first = frames - ATT * (it + 1)
        feature = x_ref[pl.ds(HALO + first, ATT)].astype(F32).reshape(ATT * tokens, chan)
        normed = ((feature - mean) * scale + shift).astype(BF16)
        qkv = (dot(normed, qkv_w) + qkv_b).astype(BF16)
        mixed = []
        for f in range(ATT):
            mine = slice(f * tokens, (f + 1) * tokens)
            scores = lax.dot_general(qkv[mine, :chan], qkv[mine, chan:2 * chan], (((1,), (1,)), ((), ())), preferred_element_type=F32)
            power = jnp.exp2((scores - jnp.max(scores, axis=1, keepdims=True)) * gain)
            probs = (power / jnp.sum(power, axis=1, keepdims=True)).astype(BF16)
            mixed.append(dot(probs, qkv[mine, 2 * chan:]).astype(BF16))
        branch = (dot(jnp.concatenate(mixed, axis=0), aw_ref[3]) + out_b).astype(BF16)
        value = (feature + branch.astype(F32)).astype(BF16)
        x_ref[pl.ds(HALO + first, ATT)] = value.reshape(ATT, height, width, chan)

        @pl.when(it == max(1, HALO // ATT))
        def _():
            send_halo(2, x_ref)

        value = value.astype(F32)
        return sums[0] + vreg_sum(value), sums[1] + vreg_sum(value * value)

    sums = lax.fori_loop(0, frames // ATT, attend, (zero, zero))
    coef = exchange(3, sums)
    take_halo(2, x_ref)
    sums = conv_stage(2, x_ref, coef, into_h, send_first(3, h_ref))
    coef = exchange(4, sums)
    take_halo(3, h_ref)
    conv_stage(3, h_ref, coef, into_x, write_out)
    for it in range(tiles // 2):
        out_copy(it).wait()


def solution(mesh):
    n_dev = mesh.shape["time"]
    video_spec = P(("batch", "time"), None, None, None)

    def device_body(latent, conv_w, conv_b, norm_g, norm_b, attn_w, attn_b):
        frames, height, width, chan = latent.shape
        anywhere = pl.BlockSpec(memory_space=pl.ANY)
        padded = (frames + HALO, height, width, chan)
        tile_shape = (height, TILE + HALO, width, 3 * chan)
        dma = pltpu.SemaphoreType.DMA
        return pl.pallas_call(
            functools.partial(kernel, n_dev),
            out_shape=jax.ShapeDtypeStruct(latent.shape, latent.dtype),
            in_specs=[anywhere] * 7,
            out_specs=anywhere,
            scratch_shapes=[
                pltpu.VMEM(padded, BF16),
                pltpu.VMEM(padded, BF16),
                pltpu.VMEM(tile_shape, BF16),
                pltpu.VMEM(tile_shape, BF16),
                pltpu.VMEM(conv_w.shape, BF16),
                pltpu.VMEM(attn_w.shape, BF16),
                pltpu.VMEM(conv_b.shape, F32),
                pltpu.VMEM(norm_g.shape, F32),
                pltpu.VMEM(norm_b.shape, F32),
                pltpu.VMEM(attn_b.shape, F32),
                pltpu.VMEM((4, HALO, height, width, chan), BF16),
                pltpu.VMEM((5, n_dev, 8, chan), F32),
                dma((CHUNKS,)),
                dma((6,)),
                dma((frames // TILE // 2,)),
                dma((4,)),
                dma((4,)),
                dma((5, n_dev)),
                dma((5, n_dev)),
            ],
            compiler_params=pltpu.CompilerParams(collective_id=0, has_side_effects=True),
        )(latent, conv_w, conv_b, norm_g, norm_b, attn_w, attn_b)

    return jax.shard_map(device_body, mesh=mesh, in_specs=(video_spec, P(), P(), P(), P(), P(), P()), out_specs=video_spec, check_vma=False)
```

```python
import functools

import jax
import jax.numpy as jnp
from jax import lax
from jax.experimental import pallas as pl
from jax.experimental.pallas import tpu as pltpu
from jax.sharding import PartitionSpec as P

GROUPS = 32
NORM_EPS = 1e-6
TILE = 8
ATT = 8
CHUNKS = 4
HALO = 2
MESH_ID = pl.DeviceIdType.MESH
F32, BF16 = jnp.float32, jnp.bfloat16


def dot(a, b):
    return jnp.dot(a, b, preferred_element_type=F32)


def vreg_sum(value):
    return jnp.sum(value.reshape(-1, 8, value.shape[-1]), axis=0)


def kernel(n_dev, latent, conv_w, conv_b, norm_g, norm_b, attn_w, attn_b, out, x_ref, h_ref, ua, ub, act_a, act_b, w_ref, aw_ref, cb_ref, g_ref, b_ref, ab_ref, halo, stats, in_sem, par_sem, out_sem, halo_send, halo_recv, stat_send, stat_recv):
    frames, height, width, chan = latent.shape
    me = lax.axis_index("time")
    tiles = frames // TILE
    piece = frames // CHUNKS
    elem_count = n_dev * frames * height * width * (chan // GROUPS)

    in_copies = [pltpu.make_async_copy(latent.at[pl.ds(c * piece, piece)], x_ref.at[pl.ds(HALO + c * piece, piece)], in_sem.at[c]) for c in range(CHUNKS)]
    for c in reversed(range(CHUNKS)):
        in_copies[c].start()
    pairs = [(norm_g, g_ref), (norm_b, b_ref), (conv_b, cb_ref), (attn_w, aw_ref), (attn_b, ab_ref), (conv_w, w_ref)]
    par_copies = [pltpu.make_async_copy(src, dst, par_sem.at[i]) for i, (src, dst) in enumerate(pairs)]
    for copy in par_copies:
        copy.start()

    barrier = pltpu.get_barrier_semaphore()
    for k in range(1, n_dev):
        pl.semaphore_signal(barrier, inc=1, device_id={"time": lax.rem(me + k, n_dev)}, device_id_type=MESH_ID)
    with jax.named_scope('barrier'):
        pl.semaphore_wait(barrier, n_dev - 1)

    def halo_copy(slot, src, start):
        return pltpu.make_async_remote_copy(src_ref=src.at[pl.ds(start, HALO)], dst_ref=halo.at[slot], send_sem=halo_send.at[slot], recv_sem=halo_recv.at[slot], device_id={"time": lax.rem(me + 1, n_dev)}, device_id_type=MESH_ID)

    def send_halo(slot, src):
        @pl.when(me < n_dev - 1)
        def _():
            halo_copy(slot, src, frames).start()

    def take_halo(slot, src):
        @pl.when(me > 0)
        def _():
            halo_copy(slot, src, frames).wait_recv()
            src[pl.ds(0, HALO)] = halo[slot]

        @pl.when(me == 0)
        def _():
            for f in range(HALO):
                src[f] = src[HALO]

        @pl.when(me < n_dev - 1)
        def _():
            halo_copy(slot, src, frames).wait_send()

    lane = lax.broadcasted_iota(jnp.int32, (8, chan), 1)

    def exchange(stage, sums):
        both = jnp.concatenate([jnp.sum(sums[0], axis=0, keepdims=True), jnp.sum(sums[1], axis=0, keepdims=True), jnp.zeros((6, chan), F32)], axis=0)
        stats[stage, me] = both

        def copy_to(k):
            return pltpu.make_async_remote_copy(src_ref=stats.at[stage, me], dst_ref=stats.at[stage, me], send_sem=stat_send.at[stage, k], recv_sem=stat_recv.at[stage, n_dev - k], device_id={"time": lax.rem(me + k, n_dev)}, device_id_type=MESH_ID)

        def copy_from(k):
            peer = lax.rem(me + k, n_dev)
            return pltpu.make_async_remote_copy(src_ref=stats.at[stage, peer], dst_ref=stats.at[stage, peer], send_sem=stat_send.at[stage, k], recv_sem=stat_recv.at[stage, k], device_id={"time": peer}, device_id_type=MESH_ID)

        for k in range(1, n_dev):
            copy_to(k).start()
        for k in range(1, n_dev):
            copy_from(k).wait_recv()
        total = stats[stage, 0]
        for d in range(1, n_dev):
            total = total + stats[stage, d]
        for k in range(1, n_dev):
            copy_to(k).wait_send()
        per_group = chan // GROUPS
        step = 1
        while step < per_group:
            swap = jnp.where(lax.rem(lane, 2 * step) < step, pltpu.roll(total, chan - step, 1), pltpu.roll(total, step, 1))
            total = total + swap
            step *= 2
        mean = total[0:1] / elem_count
        inv_std = lax.rsqrt(total[1:2] / elem_count - mean * mean + NORM_EPS)
        return mean, inv_std * g_ref[pl.ds(stage, 1)], b_ref[pl.ds(stage, 1)]

    block = width + 8
    for act in (act_a, act_b):
        for f in range(TILE + HALO):
            for i in range(height + 1):
                act[f, i * block:i * block + 8] = jnp.zeros((8, chan), F32)

    def norm_tile(src, dst, act, tile, coef):
        mean, scale, shift = coef
        scale, shift = 0.5 * scale, 0.5 * shift
        for f in range(TILE + HALO):
            value = src[tile * TILE + f].astype(F32)
            half = (value - mean) * scale + shift
            value = half + half * jnp.tanh(half)
            dst[:, f, :, chan:2 * chan] = value.astype(BF16)
            for i in range(height):
                act[f, i * block + 8:(i + 1) * block] = value[i]
            for i in range(height):
                for e in (0, 2):
                    moved = act[f, i * block + 7 + e:i * block + 7 + e + width]
                    dst[i, f, :, e * chan:(e + 1) * chan] = moved.astype(BF16)

    zero_w = jnp.zeros((chan, chan), BF16)

    def conv_tile(u, k, bias):
        def cols(row, first, count, e):
            return u[row, first:first + count, :, e * chan:(e + 1) * chan].reshape(count * width, chan)

        lhs, rhs = [], []
        for a in range(3):
            for e in range(3):
                for side in range(2):
                    lhs.append(jnp.concatenate([cols(g + side, a, TILE, e) for g in range(0, height, 2)], axis=0))
                    rhs.append(jnp.concatenate([w_ref[k, a, 1 + side, e], w_ref[k, a, side, e]], axis=1))
        main = dot(jnp.concatenate(lhs, axis=1), jnp.concatenate(rhs, axis=0))

        def extra(row, d):
            lhs, rhs = [], []
            for s in range(4):
                for e in range(3):
                    lhs.append(jnp.concatenate([cols(row, 2 * p + s, 1, e) for p in range(TILE // 2)], axis=0))
                    rhs.append(jnp.concatenate([w_ref[k, s, d, e] if s < 3 else zero_w, w_ref[k, s - 1, d, e] if s > 0 else zero_w], axis=1))
            return dot(jnp.concatenate(lhs, axis=1), jnp.concatenate(rhs, axis=0))

        lower = extra(2, 2)
        upper = extra(1, 0)
        rows = []
        for f in range(TILE):
            here = slice(f * width, (f + 1) * width)
            there = slice((TILE + f) * width, (TILE + f + 1) * width)
            pair = slice((f // 2) * width, (f // 2 + 1) * width)
            half = slice((f % 2) * chan, (f % 2 + 1) * chan)
            rows.append([main[here, :chan] + bias, main[here, chan:] + lower[pair, half] + bias, main[there, :chan] + upper[pair, half] + bias, main[there, chan:] + bias])
        return rows

    def conv_stage(k, src, coef, emit, after):
        bias = cb_ref[pl.ds(k, 1)]
        with jax.named_scope('norm_first'):
            norm_tile(src, ua, act_a, tiles - 1, coef)

        def finish(u, tile, sums):
            rows = conv_tile(u, k, bias)
            for f in range(TILE):
                for i in range(height):
                    value = emit(tile * TILE + f, i, rows[f][i].astype(BF16)).astype(F32)
                    sums = (sums[0] + vreg_sum(value), sums[1] + vreg_sum(value * value))
            return sums

        def body(it, sums):
            high = tiles - 1 - 2 * it
            norm_tile(src, ub, act_b, high - 1, coef)
            sums = finish(ua, high, sums)
            norm_tile(src, ua, act_a, jnp.maximum(high - 2, 0), coef)
            sums = finish(ub, high - 1, sums)
            after(it, high)
            return sums

        zero = jnp.zeros((8, chan), F32)
        return lax.fori_loop(0, tiles // 2, body, (zero, zero))

    def into_h(frame, i, value):
        h_ref[HALO + frame, i] = value
        return value

    def into_x(frame, i, value):
        value = (x_ref[HALO + frame, i].astype(F32) + value.astype(F32)).astype(BF16)
        x_ref[HALO + frame, i] = value
        return value

    def send_first(slot, src):
        def after(it, high):
            @pl.when(it == 0)
            def _():
                send_halo(slot, src)
        return after

    def nothing(it, high):
        pass

    def out_copy(it):
        first = frames - 2 * TILE * (it + 1)
        return pltpu.make_async_copy(x_ref.at[pl.ds(HALO + first, 2 * TILE)], out.at[pl.ds(first, 2 * TILE)], out_sem.at[it])

    def write_out(it, high):
        out_copy(it).start()

    zero = jnp.zeros((8, chan), F32)
    sums = (zero, zero)
    for c in reversed(range(CHUNKS)):
        in_copies[c].wait()
        if c == CHUNKS - 1:
            send_halo(0, x_ref)

        def add_frame(f, sums):
            value = x_ref[HALO + c * piece + f].astype(F32)
            return sums[0] + vreg_sum(value), sums[1] + vreg_sum(value * value)

        sums = lax.fori_loop(0, piece, add_frame, sums)
    with jax.named_scope('par_wait'):
        for copy in par_copies:
            copy.wait()

    with jax.named_scope('exchange0'):
        coef = exchange(0, sums)
    with jax.named_scope('halo0'):
        take_halo(0, x_ref)
    with jax.named_scope('conv0'):
        sums = conv_stage(0, x_ref, coef, into_h, send_first(1, h_ref))
    with jax.named_scope('exchange1'):
        coef = exchange(1, sums)
    with jax.named_scope('halo1'):
        take_halo(1, h_ref)
    with jax.named_scope('conv1'):
        sums = conv_stage(1, h_ref, coef, into_x, nothing)
    with jax.named_scope('exchange2'):
        mean, scale, shift = exchange(2, sums)

    tokens = height * width
    qkv_w = jnp.concatenate([aw_ref[0], aw_ref[1], aw_ref[2]], axis=1)
    qkv_b = jnp.concatenate([ab_ref[0:1], ab_ref[1:2], ab_ref[2:3]], axis=1)
    out_b = ab_ref[3:4]
    gain = chan ** -0.5 * 1.4426950408889634

    def attend(it, sums):
        first = frames - ATT * (it + 1)
        feature = x_ref[pl.ds(HALO + first, ATT)].astype(F32).reshape(ATT * tokens, chan)
        normed = ((feature - mean) * scale + shift).astype(BF16)
        qkv = (dot(normed, qkv_w) + qkv_b).astype(BF16)
        mixed = []
        for f in range(ATT):
            mine = slice(f * tokens, (f + 1) * tokens)
            scores = lax.dot_general(qkv[mine, :chan], qkv[mine, chan:2 * chan], (((1,), (1,)), ((), ())), preferred_element_type=F32)
            power = jnp.exp2((scores - jnp.max(scores, axis=1, keepdims=True)) * gain)
            probs = (power / jnp.sum(power, axis=1, keepdims=True)).astype(BF16)
            mixed.append(dot(probs, qkv[mine, 2 * chan:]).astype(BF16))
        branch = (dot(jnp.concatenate(mixed, axis=0), aw_ref[3]) + out_b).astype(BF16)
        value = (feature + branch.astype(F32)).astype(BF16)
        x_ref[pl.ds(HALO + first, ATT)] = value.reshape(ATT, height, width, chan)

        @pl.when(it == max(1, HALO // ATT))
        def _():
            send_halo(2, x_ref)

        value = value.astype(F32)
        return sums[0] + vreg_sum(value), sums[1] + vreg_sum(value * value)

    with jax.named_scope('attention'):
        sums = lax.fori_loop(0, frames // ATT, attend, (zero, zero))
    with jax.named_scope('exchange3'):
        coef = exchange(3, sums)
    with jax.named_scope('halo2'):
        take_halo(2, x_ref)
    with jax.named_scope('conv2'):
        sums = conv_stage(2, x_ref, coef, into_h, send_first(3, h_ref))
    with jax.named_scope('exchange4'):
        coef = exchange(4, sums)
    with jax.named_scope('halo3'):
        take_halo(3, h_ref)
    with jax.named_scope('conv3'):
        conv_stage(3, h_ref, coef, into_x, write_out)
    with jax.named_scope('drain'):
        for it in range(tiles // 2):
            out_copy(it).wait()


def solution(mesh):
    n_dev = mesh.shape["time"]
    video_spec = P(("batch", "time"), None, None, None)

    def device_body(latent, conv_w, conv_b, norm_g, norm_b, attn_w, attn_b):
        frames, height, width, chan = latent.shape
        anywhere = pl.BlockSpec(memory_space=pl.ANY)
        padded = (frames + HALO, height, width, chan)
        tile_shape = (height, TILE + HALO, width, 3 * chan)
        act_shape = (TILE + HALO, height * (width + 8) + 8, chan)
        dma = pltpu.SemaphoreType.DMA
        return pl.pallas_call(
            functools.partial(kernel, n_dev),
            out_shape=jax.ShapeDtypeStruct(latent.shape, latent.dtype),
            in_specs=[anywhere] * 7,
            out_specs=anywhere,
            scratch_shapes=[
                pltpu.VMEM(padded, BF16),
                pltpu.VMEM(padded, BF16),
                pltpu.VMEM(tile_shape, BF16),
                pltpu.VMEM(tile_shape, BF16),
                pltpu.VMEM(act_shape, F32),
                pltpu.VMEM(act_shape, F32),
                pltpu.VMEM(conv_w.shape, BF16),
                pltpu.VMEM(attn_w.shape, BF16),
                pltpu.VMEM(conv_b.shape, F32),
                pltpu.VMEM(norm_g.shape, F32),
                pltpu.VMEM(norm_b.shape, F32),
                pltpu.VMEM(attn_b.shape, F32),
                pltpu.VMEM((4, HALO, height, width, chan), BF16),
                pltpu.VMEM((5, n_dev, 8, chan), F32),
                dma((CHUNKS,)),
                dma((6,)),
                dma((frames // TILE // 2,)),
                dma((4,)),
                dma((4,)),
                dma((5, n_dev)),
                dma((5, n_dev)),
            ],
            compiler_params=pltpu.CompilerParams(collective_id=0, has_side_effects=True),
        )(latent, conv_w, conv_b, norm_g, norm_b, attn_w, attn_b)

    return jax.shard_map(device_body, mesh=mesh, in_specs=(video_spec, P(), P(), P(), P(), P(), P()), out_specs=video_spec, check_vma=False)
```

```python
import functools

import jax
import jax.numpy as jnp
from jax import lax
from jax.experimental import pallas as pl
from jax.experimental.pallas import tpu as pltpu
from jax.sharding import PartitionSpec as P

GROUPS = 32
NORM_EPS = 1e-6
TILE = 8
ATT = 24
CHUNKS = 4
HALO = 2
VMEM_LIMIT = 34 * 2**20
MESH_ID = pl.DeviceIdType.MESH
F32, BF16 = jnp.float32, jnp.bfloat16


def dot(a, b):
    return jnp.dot(a, b, preferred_element_type=F32)


def vreg_sum(value):
    return jnp.sum(value.reshape(-1, 8, value.shape[-1]), axis=0)


def add_sums(sums, value):
    return sums[0] + vreg_sum(value), sums[1] + vreg_sum(value * value)


def clear_act(acts, height, width):
    for act in acts:
        for f in range(act.shape[0]):
            for i in range(height + 1):
                act[f, i * (width + 8):i * (width + 8) + 8] = jnp.zeros((8, act.shape[2]), F32)


def norm_tile(src, dst, act, tile, coef):
    height, width, chan = src.shape[1:]
    block = width + 8
    mean, scale, shift = coef
    scale, shift = 0.5 * scale, 0.5 * shift
    for f in range(TILE + HALO):
        half = (src[tile * TILE + f].astype(F32) - mean) * scale + shift
        value = half + half * jnp.tanh(half)
        dst[:, f, :, chan:2 * chan] = value.astype(BF16)
        for i in range(height):
            act[f, i * block + 8:(i + 1) * block] = value[i]
        for i in range(height):
            for e in (0, 2):
                moved = act[f, i * block + 7 + e:i * block + 7 + e + width]
                dst[i, f, :, e * chan:(e + 1) * chan] = moved.astype(BF16)


def conv_tile(u, w, bias):
    height, _, width, chan = u.shape
    chan //= 3
    zero_w = jnp.zeros((chan, chan), BF16)

    def cols(row, first, count, e):
        return u[row, first:first + count, :, e * chan:(e + 1) * chan].reshape(count * width, chan)

    lhs, rhs = [], []
    for a in range(3):
        for e in range(3):
            for side in range(2):
                lhs.append(jnp.concatenate([cols(g + side, a, TILE, e) for g in range(0, height, 2)], axis=0))
                rhs.append(jnp.concatenate([w[a, 1 + side, e], w[a, side, e]], axis=1))
    main = dot(jnp.concatenate(lhs, axis=1), jnp.concatenate(rhs, axis=0))

    def extra(row, d):
        lhs, rhs = [], []
        for s in range(4):
            for e in range(3):
                lhs.append(jnp.concatenate([cols(row, 2 * p + s, 1, e) for p in range(TILE // 2)], axis=0))
                rhs.append(jnp.concatenate([w[s, d, e] if s < 3 else zero_w, w[s - 1, d, e] if s > 0 else zero_w], axis=1))
        return dot(jnp.concatenate(lhs, axis=1), jnp.concatenate(rhs, axis=0))

    lower = extra(2, 2)
    upper = extra(1, 0)
    rows = []
    for f in range(TILE):
        here = slice(f * width, (f + 1) * width)
        there = slice((TILE + f) * width, (TILE + f + 1) * width)
        pair = slice((f // 2) * width, (f // 2 + 1) * width)
        half = slice((f % 2) * chan, (f % 2 + 1) * chan)
        rows.append([main[here, :chan] + bias, main[here, chan:] + lower[pair, half] + bias, main[there, :chan] + upper[pair, half] + bias, main[there, chan:] + bias])
    return rows


def conv_stage(src, w, bias, coef, bufs, carry, emit, after):
    ua, ub, act_a, act_b = bufs
    tiles = (src.shape[0] - HALO) // TILE
    norm_tile(src, ua, act_a, tiles - 1, coef)

    def finish(u, tile, carry):
        rows = conv_tile(u, w, bias)
        for f in range(TILE):
            for i in range(len(rows[f])):
                carry = emit(tile * TILE + f, i, rows[f][i].astype(BF16), carry)
        return carry

    def body(it, carry):
        high = tiles - 1 - 2 * it
        norm_tile(src, ub, act_b, high - 1, coef)
        carry = finish(ua, high, carry)
        norm_tile(src, ua, act_a, jnp.maximum(high - 2, 0), coef)
        carry = finish(ub, high - 1, carry)
        after(it)
        return carry

    return lax.fori_loop(0, tiles // 2, body, carry)


def kernel(n_dev, latent, conv_w, conv_b, norm_g, norm_b, attn_w, attn_b, x_ref, h_ref, w_last, aux, ua, ub, act_a, act_b, qkv, probs, w_ref, aw_ref, cb_ref, g_ref, b_ref, ab_ref, halo, stats, in_sem, par_sem, halo_send, halo_recv, stat_send, stat_recv):
    frames, height, width, chan = latent.shape
    convs = conv_w.shape[0]
    tokens = height * width
    me = lax.axis_index("time")
    piece = frames // CHUNKS
    elem_count = n_dev * frames * tokens * (chan // GROUPS)
    bufs = (ua, ub, act_a, act_b)

    in_copies = [pltpu.make_async_copy(latent.at[pl.ds(c * piece, piece)], x_ref.at[pl.ds(HALO + c * piece, piece)], in_sem.at[c]) for c in range(CHUNKS)]
    for c in reversed(range(CHUNKS)):
        in_copies[c].start()
    barrier = pltpu.get_barrier_semaphore()
    for k in range(1, n_dev):
        pl.semaphore_signal(barrier, inc=1, device_id={"time": lax.rem(me + k, n_dev)}, device_id_type=MESH_ID)
    pairs = [(norm_g, g_ref), (norm_b, b_ref), (conv_b, cb_ref), (attn_w, aw_ref), (attn_b, ab_ref), (conv_w.at[pl.ds(0, convs - 1)], w_ref), (conv_w.at[convs - 1], w_last)]
    par_copies = [pltpu.make_async_copy(src, dst, par_sem.at[i]) for i, (src, dst) in enumerate(pairs)]
    for copy in par_copies:
        copy.start()
    clear_act((act_a, act_b), height, width)

    def halo_copy(slot, src):
        return pltpu.make_async_remote_copy(src_ref=src.at[pl.ds(frames, HALO)], dst_ref=halo.at[slot], send_sem=halo_send.at[slot], recv_sem=halo_recv.at[slot], device_id={"time": lax.rem(me + 1, n_dev)}, device_id_type=MESH_ID)

    def send_halo(slot, src):
        @pl.when(me < n_dev - 1)
        def _():
            halo_copy(slot, src).start()

    def take_halo(slot, src):
        @pl.when(me > 0)
        def _():
            halo_copy(slot, src).wait_recv()
            src[pl.ds(0, HALO)] = halo[slot]

        @pl.when(me == 0)
        def _():
            for f in range(HALO):
                src[f] = src[HALO]

        @pl.when(me < n_dev - 1)
        def _():
            halo_copy(slot, src).wait_send()

    lane = lax.broadcasted_iota(jnp.int32, (2, chan), 1)

    def exchange(stage, sums):
        stats[stage, me] = jnp.concatenate([jnp.sum(part, axis=0, keepdims=True) for part in sums], axis=0)

        def copy_to(k):
            return pltpu.make_async_remote_copy(src_ref=stats.at[stage, me], dst_ref=stats.at[stage, me], send_sem=stat_send.at[stage, k], recv_sem=stat_recv.at[stage, n_dev - k], device_id={"time": lax.rem(me + k, n_dev)}, device_id_type=MESH_ID)

        def copy_from(k):
            peer = lax.rem(me + k, n_dev)
            return pltpu.make_async_remote_copy(src_ref=stats.at[stage, peer], dst_ref=stats.at[stage, peer], send_sem=stat_send.at[stage, k], recv_sem=stat_recv.at[stage, k], device_id={"time": peer}, device_id_type=MESH_ID)

        for k in range(1, n_dev):
            copy_to(k).start()
        for k in range(1, n_dev):
            copy_from(k).wait_recv()
        total = stats[stage, 0]
        for d in range(1, n_dev):
            total = total + stats[stage, d]
        for k in range(1, n_dev):
            copy_to(k).wait_send()
        per_group = chan // GROUPS
        step = 1
        while step < per_group:
            swap = jnp.where(lax.rem(lane, 2 * step) < step, pltpu.roll(total, chan - step, 1), pltpu.roll(total, step, 1))
            total = total + swap
            step *= 2
        mean = total[0:1] / elem_count
        inv_std = lax.rsqrt(total[1:2] / elem_count - mean * mean + NORM_EPS)
        return mean, inv_std * g_ref[pl.ds(stage, 1)], b_ref[pl.ds(stage, 1)]

    def into(ref):
        def emit(frame, i, value, sums):
            ref[HALO + frame, i] = value
            return add_sums(sums, value.astype(F32))
        return emit

    def into_x(frame, i, value, sums):
        value = (x_ref[HALO + frame, i].astype(F32) + value.astype(F32)).astype(BF16)
        x_ref[HALO + frame, i] = value
        return add_sums(sums, value.astype(F32))

    def send_first(slot, src):
        def after(it):
            @pl.when(it == 0)
            def _():
                send_halo(slot, src)
        return after

    zero = jnp.zeros((8, chan), F32)
    sums = (zero, zero)
    for c in reversed(range(CHUNKS)):
        in_copies[c].wait()

        def add_frame(f, sums):
            return add_sums(sums, x_ref[HALO + c * piece + f].astype(F32))

        sums = lax.fori_loop(0, piece, add_frame, sums)
    with jax.named_scope("barrier"):
        pl.semaphore_wait(barrier, n_dev - 1)
    send_halo(0, x_ref)
    with jax.named_scope("par_wait"):
        for copy in par_copies:
            copy.wait()

    def conv(k, src, emit, after, coef):
        with jax.named_scope("conv"):
            return conv_stage(src, w_ref.at[k], cb_ref[pl.ds(k, 1)], coef, bufs, (zero, zero), emit, after)

    def renorm(stage, sums):
        with jax.named_scope("exchange"):
            return exchange(stage, sums)

    coef = renorm(0, sums)
    take_halo(0, x_ref)
    sums = conv(0, x_ref, into(h_ref), send_first(1, h_ref), coef)
    coef = renorm(1, sums)
    take_halo(1, h_ref)
    sums = conv(1, h_ref, into_x, lambda it: None, coef)
    mean, scale, shift = renorm(2, sums)

    qkv_w = jnp.concatenate([aw_ref[0], aw_ref[1], aw_ref[2]], axis=1)
    qkv_bias = jnp.concatenate([ab_ref[0:1], ab_ref[1:2], ab_ref[2:3]], axis=1)
    out_bias = ab_ref[3:4]
    gain = chan ** -0.5 * 1.4426950408889634
    pairs = ATT // 2

    def attend(it, sums):
        first = HALO + frames - ATT * (it + 1)
        scores, mixed = {}, {}

        def project(p):
            feature = x_ref[pl.ds(first + 2 * p, 2)].astype(F32).reshape(2 * tokens, chan)
            normed = ((feature - mean) * scale + shift).astype(BF16)
            qkv[p % 3] = (dot(normed, qkv_w) + qkv_bias).astype(BF16)

        def score(p):
            for f in range(2):
                mine = slice(f * tokens, (f + 1) * tokens)
                scores[p, f] = lax.dot_general(qkv[p % 3, mine, :chan], qkv[p % 3, mine, chan:2 * chan], (((1,), (1,)), ((), ())), preferred_element_type=F32)

        def softmax(p):
            for f in range(2):
                value = scores.pop((p, f))
                power = jnp.exp2((value - jnp.max(value, axis=1, keepdims=True)) * gain)
                probs[p % 2, f] = (power / jnp.sum(power, axis=1, keepdims=True)).astype(BF16)

        def mix(p):
            for f in range(2):
                mixed[p, f] = dot(probs[p % 2, f], qkv[p % 3, f * tokens:(f + 1) * tokens, 2 * chan:]).astype(BF16)

        def close(p, sums):
            branch = (dot(jnp.concatenate([mixed.pop((p, f)) for f in range(2)], axis=0), aw_ref[3]) + out_bias).astype(BF16)
            value = (x_ref[pl.ds(first + 2 * p, 2)].astype(F32).reshape(2 * tokens, chan) + branch.astype(F32)).astype(BF16)
            h_ref[pl.ds(first + 2 * p, 2)] = value.reshape(2, height, width, chan)
            return add_sums(sums, value.astype(F32))

        for step in range(pairs + 3):
            if 0 <= step - 1 < pairs:
                score(step - 1)
            if step < pairs:
                project(step)
            if 0 <= step - 2 < pairs:
                mix(step - 2)
            if 0 <= step - 1 < pairs:
                softmax(step - 1)
            if 0 <= step - 3 < pairs:
                sums = close(step - 3, sums)

        @pl.when(it == 0)
        def _():
            send_halo(2, h_ref)

        return sums

    with jax.named_scope("attention"):
        sums = lax.fori_loop(0, frames // ATT, attend, (zero, zero))
    coef = renorm(3, sums)
    take_halo(2, h_ref)
    sums = conv(2, h_ref, into(x_ref), send_first(3, x_ref), coef)
    coef = renorm(4, sums)
    take_halo(3, x_ref)
    aux[0:4] = jnp.concatenate([*coef, cb_ref[convs - 1:convs]], axis=0)


def last_kernel(h_ref, x_ref, w_ref, aux, out, y_ref, ua, ub, act_a, act_b, out_sem):
    frames, height, width, chan = y_ref.shape
    clear_act((act_a, act_b), height, width)
    coef = (aux[0:1], aux[1:2], aux[2:3])

    def out_copy(it):
        first = frames - 2 * TILE * (it + 1)
        return pltpu.make_async_copy(y_ref.at[pl.ds(first, 2 * TILE)], out.at[pl.ds(first, 2 * TILE)], out_sem.at[it])

    def into_y(frame, i, value, carry):
        y_ref[frame, i] = (x_ref[HALO + frame, i].astype(F32) + value.astype(F32)).astype(BF16)
        return carry

    with jax.named_scope("conv_last"):
        conv_stage(h_ref, w_ref, aux[3:4], coef, (ua, ub, act_a, act_b), 0, into_y, lambda it: out_copy(it).start())
    with jax.named_scope("drain"):
        for it in range(frames // TILE // 2):
            out_copy(it).wait()


def solution(mesh):
    n_dev = mesh.shape["time"]
    video_spec = P(("batch", "time"), None, None, None)

    def device_body(latent, conv_w, conv_b, norm_g, norm_b, attn_w, attn_b):
        frames, height, width, chan = latent.shape
        convs = conv_w.shape[0]
        hbm, vmem = pl.BlockSpec(memory_space=pltpu.HBM), pl.BlockSpec(memory_space=pltpu.VMEM)
        padded = (frames + HALO, height, width, chan)
        dma = pltpu.SemaphoreType.DMA
        bufs = [pltpu.VMEM((height, TILE + HALO, width, 3 * chan), BF16)] * 2 + [pltpu.VMEM((TILE + HALO, height * (width + 8) + 8, chan), F32)] * 2
        state = pl.pallas_call(
            functools.partial(kernel, n_dev),
            out_shape=[pltpu.VMEM(padded, BF16), pltpu.VMEM(padded, BF16), pltpu.VMEM(conv_w.shape[1:], BF16), pltpu.VMEM((8, chan), F32)],
            in_specs=[hbm] * 7,
            out_specs=[vmem] * 4,
            scratch_shapes=[
                *bufs,
                pltpu.VMEM((3, 2 * height * width, 3 * chan), BF16),
                pltpu.VMEM((2, 2, height * width, height * width), BF16),
                pltpu.VMEM((convs - 1, *conv_w.shape[1:]), BF16),
                pltpu.VMEM(attn_w.shape, BF16),
                pltpu.VMEM(conv_b.shape, F32),
                pltpu.VMEM(norm_g.shape, F32),
                pltpu.VMEM(norm_b.shape, F32),
                pltpu.VMEM(attn_b.shape, F32),
                pltpu.VMEM((4, HALO, height, width, chan), BF16),
                pltpu.VMEM((5, n_dev, 2, chan), F32),
                dma((CHUNKS,)),
                dma((7,)),
                dma((4,)),
                dma((4,)),
                dma((5, n_dev)),
                dma((5, n_dev)),
            ],
            compiler_params=pltpu.CompilerParams(collective_id=0, has_side_effects=True, vmem_limit_bytes=VMEM_LIMIT),
        )(latent, conv_w, conv_b, norm_g, norm_b, attn_w, attn_b)
        return pl.pallas_call(
            last_kernel,
            out_shape=jax.ShapeDtypeStruct(latent.shape, latent.dtype),
            in_specs=[vmem] * 4,
            out_specs=hbm,
            scratch_shapes=[pltpu.VMEM(latent.shape, BF16), *bufs, dma((frames // TILE // 2,))],
            compiler_params=pltpu.CompilerParams(vmem_limit_bytes=VMEM_LIMIT),
        )(*state)

    return jax.shard_map(device_body, mesh=mesh, in_specs=(video_spec, P(), P(), P(), P(), P(), P()), out_specs=video_spec, check_vma=False)
```

```python
import functools

import jax
import jax.numpy as jnp
from jax import lax
from jax.experimental import pallas as pl
from jax.experimental.pallas import tpu as pltpu
from jax.sharding import PartitionSpec as P

GROUPS = 32
NORM_EPS = 1e-6
TILE = 8
ATT = 24
CHUNKS = 4
HALO = 2
VMEM_LIMIT = 34 * 2**20
MESH_ID = pl.DeviceIdType.MESH
F32, BF16 = jnp.float32, jnp.bfloat16


def dot(a, b):
    return jnp.dot(a, b, preferred_element_type=F32)


def vreg_sum(value):
    return jnp.sum(value.reshape(-1, 8, value.shape[-1]), axis=0)


def add_sums(sums, value):
    return sums[0] + vreg_sum(value), sums[1] + vreg_sum(value * value)


def clear_act(acts, height, width):
    for act in acts:
        for f in range(act.shape[0]):
            for i in range(height + 1):
                act[f, i * (width + 8):i * (width + 8) + 8] = jnp.zeros((8, act.shape[2]), F32)


def norm_tile(src, dst, act, tile, coef):
    height, width, chan = src.shape[1:]
    block = width + 8
    mean, scale, shift = coef
    scale, shift = 0.5 * scale, 0.5 * shift
    for f in range(TILE + HALO):
        half = (src[tile * TILE + f].astype(F32) - mean) * scale + shift
        value = half + half * jnp.tanh(half)
        dst[:, f, :, chan:2 * chan] = value.astype(BF16)
        for i in range(height):
            act[f, i * block + 8:(i + 1) * block] = value[i]
        for i in range(height):
            for e in (0, 2):
                moved = act[f, i * block + 7 + e:i * block + 7 + e + width]
                dst[i, f, :, e * chan:(e + 1) * chan] = moved.astype(BF16)


def conv_tile(u, w, bias):
    height, _, width, chan = u.shape
    chan //= 3
    zero_w = jnp.zeros((chan, chan), BF16)

    def cols(row, first, count, e):
        return u[row, first:first + count, :, e * chan:(e + 1) * chan].reshape(count * width, chan)

    lhs, rhs = [], []
    for a in range(3):
        for e in range(3):
            for side in range(2):
                lhs.append(jnp.concatenate([cols(g + side, a, TILE, e) for g in range(0, height, 2)], axis=0))
                rhs.append(jnp.concatenate([w[a, 1 + side, e], w[a, side, e]], axis=1))
    main = dot(jnp.concatenate(lhs, axis=1), jnp.concatenate(rhs, axis=0))

    def extra(row, d):
        lhs, rhs = [], []
        for s in range(4):
            for e in range(3):
                lhs.append(jnp.concatenate([cols(row, 2 * p + s, 1, e) for p in range(TILE // 2)], axis=0))
                rhs.append(jnp.concatenate([w[s, d, e] if s < 3 else zero_w, w[s - 1, d, e] if s > 0 else zero_w], axis=1))
        return dot(jnp.concatenate(lhs, axis=1), jnp.concatenate(rhs, axis=0))

    lower = extra(2, 2)
    upper = extra(1, 0)
    rows = []
    for f in range(TILE):
        here = slice(f * width, (f + 1) * width)
        there = slice((TILE + f) * width, (TILE + f + 1) * width)
        pair = slice((f // 2) * width, (f // 2 + 1) * width)
        half = slice((f % 2) * chan, (f % 2 + 1) * chan)
        rows.append([main[here, :chan] + bias, main[here, chan:] + lower[pair, half] + bias, main[there, :chan] + upper[pair, half] + bias, main[there, chan:] + bias])
    return rows


def conv_stage(src, w, bias, coef, bufs, carry, emit, after):
    ua, ub, act_a, act_b = bufs
    tiles = (src.shape[0] - HALO) // TILE
    norm_tile(src, ua, act_a, tiles - 1, coef)

    def finish(u, tile, carry):
        rows = conv_tile(u, w, bias)
        for f in range(TILE):
            for i in range(len(rows[f])):
                carry = emit(tile * TILE + f, i, rows[f][i].astype(BF16), carry)
        return carry

    def body(it, carry):
        high = tiles - 1 - 2 * it
        norm_tile(src, ub, act_b, high - 1, coef)
        carry = finish(ua, high, carry)
        norm_tile(src, ua, act_a, jnp.maximum(high - 2, 0), coef)
        carry = finish(ub, high - 1, carry)
        after(it)
        return carry

    return lax.fori_loop(0, tiles // 2, body, carry)


def kernel(n_dev, latent, conv_w, conv_b, norm_g, norm_b, attn_w, attn_b, x_ref, h_ref, w_last, aux, ua, ub, act_a, act_b, qkv, probs, w_ref, aw_ref, cb_ref, g_ref, b_ref, ab_ref, halo, stats, in_sem, par_sem, halo_send, halo_recv, stat_send, stat_recv):
    frames, height, width, chan = latent.shape
    convs = conv_w.shape[0]
    tokens = height * width
    me = lax.axis_index("time")
    piece = frames // CHUNKS
    elem_count = n_dev * frames * tokens * (chan // GROUPS)
    bufs = (ua, ub, act_a, act_b)

    in_copies = [pltpu.make_async_copy(latent.at[pl.ds(c * piece, piece)], x_ref.at[pl.ds(HALO + c * piece, piece)], in_sem.at[c]) for c in range(CHUNKS)]
    for c in reversed(range(CHUNKS)):
        in_copies[c].start()
    barrier = pltpu.get_barrier_semaphore()
    for k in range(1, n_dev):
        pl.semaphore_signal(barrier, inc=1, device_id={"time": lax.rem(me + k, n_dev)}, device_id_type=MESH_ID)
    pairs = [(norm_g, g_ref), (norm_b, b_ref), (conv_b, cb_ref), (attn_w, aw_ref), (attn_b, ab_ref), (conv_w.at[pl.ds(0, convs - 1)], w_ref), (conv_w.at[convs - 1], w_last)]
    par_copies = [pltpu.make_async_copy(src, dst, par_sem.at[i]) for i, (src, dst) in enumerate(pairs)]
    for copy in par_copies:
        copy.start()
    clear_act((act_a, act_b), height, width)

    def halo_copy(slot, src):
        return pltpu.make_async_remote_copy(src_ref=src.at[pl.ds(frames, HALO)], dst_ref=halo.at[slot], send_sem=halo_send.at[slot], recv_sem=halo_recv.at[slot], device_id={"time": lax.rem(me + 1, n_dev)}, device_id_type=MESH_ID)

    def send_halo(slot, src):
        @pl.when(me < n_dev - 1)
        def _():
            halo_copy(slot, src).start()

    def take_halo(slot, src):
        @pl.when(me > 0)
        def _():
            halo_copy(slot, src).wait_recv()
            src[pl.ds(0, HALO)] = halo[slot]

        @pl.when(me == 0)
        def _():
            for f in range(HALO):
                src[f] = src[HALO]

        @pl.when(me < n_dev - 1)
        def _():
            halo_copy(slot, src).wait_send()

    lane = lax.broadcasted_iota(jnp.int32, (2, chan), 1)

    def exchange(stage, sums):
        stats[stage, me] = jnp.concatenate([jnp.sum(part, axis=0, keepdims=True) for part in sums], axis=0)

        def copy_to(k):
            return pltpu.make_async_remote_copy(src_ref=stats.at[stage, me], dst_ref=stats.at[stage, me], send_sem=stat_send.at[stage, k], recv_sem=stat_recv.at[stage, n_dev - k], device_id={"time": lax.rem(me + k, n_dev)}, device_id_type=MESH_ID)

        def copy_from(k):
            peer = lax.rem(me + k, n_dev)
            return pltpu.make_async_remote_copy(src_ref=stats.at[stage, peer], dst_ref=stats.at[stage, peer], send_sem=stat_send.at[stage, k], recv_sem=stat_recv.at[stage, k], device_id={"time": peer}, device_id_type=MESH_ID)

        for k in range(1, n_dev):
            copy_to(k).start()
        for k in range(1, n_dev):
            copy_from(k).wait_recv()
        total = stats[stage, 0]
        for d in range(1, n_dev):
            total = total + stats[stage, d]
        for k in range(1, n_dev):
            copy_to(k).wait_send()
        per_group = chan // GROUPS
        step = 1
        while step < per_group:
            swap = jnp.where(lax.rem(lane, 2 * step) < step, pltpu.roll(total, chan - step, 1), pltpu.roll(total, step, 1))
            total = total + swap
            step *= 2
        mean = total[0:1] / elem_count
        inv_std = lax.rsqrt(total[1:2] / elem_count - mean * mean + NORM_EPS)
        return mean, inv_std * g_ref[pl.ds(stage, 1)], b_ref[pl.ds(stage, 1)]

    def into(ref):
        def emit(frame, i, value, sums):
            ref[HALO + frame, i] = value
            return add_sums(sums, value.astype(F32))
        return emit

    def into_x(frame, i, value, sums):
        value = (x_ref[HALO + frame, i].astype(F32) + value.astype(F32)).astype(BF16)
        x_ref[HALO + frame, i] = value
        return add_sums(sums, value.astype(F32))

    def send_first(slot, src):
        def after(it):
            @pl.when(it == 0)
            def _():
                send_halo(slot, src)
        return after

    zero = jnp.zeros((8, chan), F32)
    sums = (zero, zero)
    for c in reversed(range(CHUNKS)):
        in_copies[c].wait()

        def add_frame(f, sums):
            return add_sums(sums, x_ref[HALO + c * piece + f].astype(F32))

        sums = lax.fori_loop(0, piece, add_frame, sums)
    with jax.named_scope("barrier"):
        pl.semaphore_wait(barrier, n_dev - 1)
    send_halo(0, x_ref)
    with jax.named_scope("par_wait"):
        for copy in par_copies:
            copy.wait()

    def conv(k, src, emit, after, coef):
        with jax.named_scope("conv"):
            return conv_stage(src, w_ref.at[k], cb_ref[pl.ds(k, 1)], coef, bufs, (zero, zero), emit, after)

    def renorm(stage, sums):
        with jax.named_scope("exchange"):
            return exchange(stage, sums)

    coef = renorm(0, sums)
    take_halo(0, x_ref)
    sums = conv(0, x_ref, into(h_ref), send_first(1, h_ref), coef)
    coef = renorm(1, sums)
    take_halo(1, h_ref)
    sums = conv(1, h_ref, into_x, lambda it: None, coef)
    mean, scale, shift = renorm(2, sums)

    qkv_w = jnp.concatenate([aw_ref[0], aw_ref[1], aw_ref[2]], axis=1)
    qkv_bias = jnp.concatenate([ab_ref[0:1], ab_ref[1:2], ab_ref[2:3]], axis=1)
    out_bias = ab_ref[3:4]
    gain = chan ** -0.5 * 1.4426950408889634
    pairs = ATT // 2

    def attend(it, sums):
        first = HALO + frames - ATT * (it + 1)
        scores, mixed = {}, {}

        def project(p):
            feature = x_ref[pl.ds(first + 2 * p, 2)].astype(F32).reshape(2 * tokens, chan)
            normed = ((feature - mean) * scale + shift).astype(BF16)
            qkv[p % 3] = (dot(normed, qkv_w) + qkv_bias).astype(BF16)

        def score(p):
            for f in range(2):
                mine = slice(f * tokens, (f + 1) * tokens)
                scores[p, f] = lax.dot_general(qkv[p % 3, mine, :chan], qkv[p % 3, mine, chan:2 * chan], (((1,), (1,)), ((), ())), preferred_element_type=F32)

        def softmax(p):
            for f in range(2):
                value = scores.pop((p, f))
                power = jnp.exp2((value - jnp.max(value, axis=1, keepdims=True)) * gain)
                probs[p % 2, f] = (power / jnp.sum(power, axis=1, keepdims=True)).astype(BF16)

        def mix(p):
            for f in range(2):
                mixed[p, f] = dot(probs[p % 2, f], qkv[p % 3, f * tokens:(f + 1) * tokens, 2 * chan:]).astype(BF16)

        def close(p, sums):
            branch = (dot(jnp.concatenate([mixed.pop((p, f)) for f in range(2)], axis=0), aw_ref[3]) + out_bias).astype(BF16)
            value = (x_ref[pl.ds(first + 2 * p, 2)].astype(F32).reshape(2 * tokens, chan) + branch.astype(F32)).astype(BF16)
            h_ref[pl.ds(first + 2 * p, 2)] = value.reshape(2, height, width, chan)
            return add_sums(sums, value.astype(F32))

        for step in range(pairs + 3):
            if 0 <= step - 1 < pairs:
                score(step - 1)
            if step < pairs:
                project(step)
            if 0 <= step - 2 < pairs:
                mix(step - 2)
            if 0 <= step - 1 < pairs:
                softmax(step - 1)
            if 0 <= step - 3 < pairs:
                sums = close(step - 3, sums)

        @pl.when(it == 0)
        def _():
            send_halo(2, h_ref)

        return sums

    with jax.named_scope("attention"):
        sums = lax.fori_loop(0, frames // ATT, attend, (zero, zero))
    coef = renorm(3, sums)
    take_halo(2, h_ref)
    sums = conv(2, h_ref, into(x_ref), send_first(3, x_ref), coef)
    coef = renorm(4, sums)
    take_halo(3, x_ref)
    aux[0:4] = jnp.concatenate([*coef, cb_ref[convs - 1:convs]], axis=0)


def last_kernel(h_ref, x_ref, w_ref, aux, out, y_ref, ua, ub, act_a, act_b, out_sem):
    frames, height, width, chan = y_ref.shape
    clear_act((act_a, act_b), height, width)
    coef = (aux[0:1], aux[1:2], aux[2:3])

    def out_copy(it):
        first = frames - 2 * TILE * (it + 1)
        return pltpu.make_async_copy(y_ref.at[pl.ds(first, 2 * TILE)], out.at[pl.ds(first, 2 * TILE)], out_sem.at[it])

    def into_y(frame, i, value, carry):
        y_ref[frame, i] = (x_ref[HALO + frame, i].astype(F32) + value.astype(F32)).astype(BF16)
        return carry

    with jax.named_scope("conv_last"):
        conv_stage(h_ref, w_ref, aux[3:4], coef, (ua, ub, act_a, act_b), 0, into_y, lambda it: out_copy(it).start())
    with jax.named_scope("drain"):
        for it in range(frames // TILE // 2):
            out_copy(it).wait()


def solution(mesh):
    n_dev = mesh.shape["time"]
    video_spec = P(("batch", "time"), None, None, None)

    def device_body(latent, conv_w, conv_b, norm_g, norm_b, attn_w, attn_b):
        frames, height, width, chan = latent.shape
        convs = conv_w.shape[0]
        hbm, vmem = pl.BlockSpec(memory_space=pltpu.HBM), pl.BlockSpec(memory_space=pltpu.VMEM)
        padded = (frames + HALO, height, width, chan)
        dma = pltpu.SemaphoreType.DMA
        bufs = [pltpu.VMEM((height, TILE + HALO, width, 3 * chan), BF16)] * 2 + [pltpu.VMEM((TILE + HALO, height * (width + 8) + 8, chan), F32)] * 2
        state = pl.pallas_call(
            functools.partial(kernel, n_dev),
            out_shape=[pltpu.VMEM(padded, BF16), pltpu.VMEM(padded, BF16), pltpu.VMEM(conv_w.shape[1:], BF16), pltpu.VMEM((8, chan), F32)],
            in_specs=[hbm] * 7,
            out_specs=[vmem] * 4,
            scratch_shapes=[
                *bufs,
                pltpu.VMEM((3, 2 * height * width, 3 * chan), BF16),
                pltpu.VMEM((2, 2, height * width, height * width), BF16),
                pltpu.VMEM((convs - 1, *conv_w.shape[1:]), BF16),
                pltpu.VMEM(attn_w.shape, BF16),
                pltpu.VMEM(conv_b.shape, F32),
                pltpu.VMEM(norm_g.shape, F32),
                pltpu.VMEM(norm_b.shape, F32),
                pltpu.VMEM(attn_b.shape, F32),
                pltpu.VMEM((4, HALO, height, width, chan), BF16),
                pltpu.VMEM((5, n_dev, 2, chan), F32),
                dma((CHUNKS,)),
                dma((7,)),
                dma((4,)),
                dma((4,)),
                dma((5, n_dev)),
                dma((5, n_dev)),
            ],
            compiler_params=pltpu.CompilerParams(collective_id=0, has_side_effects=True, vmem_limit_bytes=VMEM_LIMIT),
        )(*(pltpu.with_memory_space_constraint(value, pltpu.HBM) for value in (latent, conv_w, conv_b, norm_g, norm_b, attn_w, attn_b)))
        return pl.pallas_call(
            last_kernel,
            out_shape=jax.ShapeDtypeStruct(latent.shape, latent.dtype),
            in_specs=[vmem] * 4,
            out_specs=hbm,
            scratch_shapes=[pltpu.VMEM(latent.shape, BF16), *bufs, dma((frames // TILE // 2,))],
            compiler_params=pltpu.CompilerParams(vmem_limit_bytes=VMEM_LIMIT),
        )(*state)

    return jax.shard_map(device_body, mesh=mesh, in_specs=(video_spec, P(), P(), P(), P(), P(), P()), out_specs=video_spec, check_vma=False)
```

```python
import functools

import jax
import jax.numpy as jnp
from jax import lax
from jax.experimental import pallas as pl
from jax.experimental.pallas import tpu as pltpu
from jax.sharding import PartitionSpec as P

GROUPS = 32
NORM_EPS = 1e-6
TILE = 8
ATT = 24
CHUNKS = 8
HALO = 2
VMEM_LIMIT = 34 * 2**20
MESH_ID = pl.DeviceIdType.MESH
F32, BF16 = jnp.float32, jnp.bfloat16


def dot(a, b):
    return jnp.dot(a, b, preferred_element_type=F32)


def vreg_sum(value):
    return jnp.sum(value.reshape(-1, 8, value.shape[-1]), axis=0)


def add_sums(sums, value):
    return sums[0] + vreg_sum(value), sums[1] + vreg_sum(value * value)


def clear_act(acts, height, width):
    for act in acts:
        for f in range(act.shape[0]):
            for i in range(height + 1):
                act[f, i * (width + 8):i * (width + 8) + 8] = jnp.zeros((8, act.shape[2]), F32)


def norm_tile(src, dst, act, tile, coef):
    height, width, chan = src.shape[1:]
    block = width + 8
    mean, scale, shift = coef
    scale, shift = 0.5 * scale, 0.5 * shift
    for f in range(TILE + HALO):
        half = (src[tile * TILE + f].astype(F32) - mean) * scale + shift
        value = half + half * jnp.tanh(half)
        dst[:, f, :, chan:2 * chan] = value.astype(BF16)
        for i in range(height):
            act[f, i * block + 8:(i + 1) * block] = value[i]
        for i in range(height):
            for e in (0, 2):
                moved = act[f, i * block + 7 + e:i * block + 7 + e + width]
                dst[i, f, :, e * chan:(e + 1) * chan] = moved.astype(BF16)


def conv_tile(u, w, bias):
    height, _, width, chan = u.shape
    chan //= 3
    zero_w = jnp.zeros((chan, chan), BF16)

    def cols(row, first, count, e):
        return u[row, first:first + count, :, e * chan:(e + 1) * chan].reshape(count * width, chan)

    lhs, rhs = [], []
    for a in range(3):
        for e in range(3):
            for side in range(2):
                lhs.append(jnp.concatenate([cols(g + side, a, TILE, e) for g in range(0, height, 2)], axis=0))
                rhs.append(jnp.concatenate([w[a, 1 + side, e], w[a, side, e]], axis=1))
    main = dot(jnp.concatenate(lhs, axis=1), jnp.concatenate(rhs, axis=0))

    def extra(row, d):
        lhs, rhs = [], []
        for s in range(4):
            for e in range(3):
                lhs.append(jnp.concatenate([cols(row, 2 * p + s, 1, e) for p in range(TILE // 2)], axis=0))
                rhs.append(jnp.concatenate([w[s, d, e] if s < 3 else zero_w, w[s - 1, d, e] if s > 0 else zero_w], axis=1))
        return dot(jnp.concatenate(lhs, axis=1), jnp.concatenate(rhs, axis=0))

    lower = extra(2, 2)
    upper = extra(1, 0)
    rows = []
    for f in range(TILE):
        here = slice(f * width, (f + 1) * width)
        there = slice((TILE + f) * width, (TILE + f + 1) * width)
        pair = slice((f // 2) * width, (f // 2 + 1) * width)
        half = slice((f % 2) * chan, (f % 2 + 1) * chan)
        rows.append([main[here, :chan] + bias, main[here, chan:] + lower[pair, half] + bias, main[there, :chan] + upper[pair, half] + bias, main[there, chan:] + bias])
    return rows


def conv_stage(src, w, bias, coef, bufs, carry, emit, after, done=lambda tile: None):
    ua, ub, act_a, act_b = bufs
    tiles = (src.shape[0] - HALO) // TILE
    norm_tile(src, ua, act_a, tiles - 1, coef)

    def finish(u, tile, carry):
        rows = conv_tile(u, w, bias)
        for f in range(TILE):
            for i in range(len(rows[f])):
                carry = emit(tile * TILE + f, i, rows[f][i].astype(BF16), carry)
        return carry

    def body(it, carry):
        high = tiles - 1 - 2 * it
        norm_tile(src, ub, act_b, high - 1, coef)
        carry = finish(ua, high, carry)
        done(high)
        norm_tile(src, ua, act_a, jnp.maximum(high - 2, 0), coef)
        carry = finish(ub, high - 1, carry)
        done(high - 1)
        after(it)
        return carry

    return lax.fori_loop(0, tiles // 2, body, carry)


def kernel(n_dev, latent, conv_w, conv_b, norm_g, norm_b, attn_w, attn_b, x_ref, h_ref, w_last, aux, ua, ub, act_a, act_b, qkv, probs, w_ref, aw_ref, cb_ref, g_ref, b_ref, ab_ref, halo, stats, in_sem, par_sem, halo_send, halo_recv, stat_send, stat_recv):
    frames, height, width, chan = latent.shape
    convs = conv_w.shape[0]
    tokens = height * width
    me = lax.axis_index("time")
    piece = frames // CHUNKS
    elem_count = n_dev * frames * tokens * (chan // GROUPS)
    bufs = (ua, ub, act_a, act_b)

    in_copies = [pltpu.make_async_copy(latent.at[pl.ds(c * piece, piece)], x_ref.at[pl.ds(HALO + c * piece, piece)], in_sem.at[c]) for c in range(CHUNKS)]
    for c in reversed(range(CHUNKS)):
        in_copies[c].start()
    barrier = pltpu.get_barrier_semaphore()
    for k in range(1, n_dev):
        pl.semaphore_signal(barrier, inc=1, device_id={"time": lax.rem(me + k, n_dev)}, device_id_type=MESH_ID)
    pairs = [(norm_g, g_ref), (norm_b, b_ref), (conv_b, cb_ref), (attn_w, aw_ref), (attn_b, ab_ref), (conv_w.at[pl.ds(0, convs - 1)], w_ref), (conv_w.at[convs - 1], w_last)]
    par_copies = [pltpu.make_async_copy(src, dst, par_sem.at[i]) for i, (src, dst) in enumerate(pairs)]
    for copy in par_copies[:-2]:
        copy.start()
    clear_act((act_a, act_b), height, width)

    def halo_copy(slot, src):
        return pltpu.make_async_remote_copy(src_ref=src.at[pl.ds(frames, HALO)], dst_ref=halo.at[slot], send_sem=halo_send.at[slot], recv_sem=halo_recv.at[slot], device_id={"time": lax.rem(me + 1, n_dev)}, device_id_type=MESH_ID)

    def send_halo(slot, src):
        @pl.when(me < n_dev - 1)
        def _():
            halo_copy(slot, src).start()

    def take_halo(slot, src):
        @pl.when(me > 0)
        def _():
            halo_copy(slot, src).wait_recv()
            src[pl.ds(0, HALO)] = halo[slot]

        @pl.when(me == 0)
        def _():
            for f in range(HALO):
                src[f] = src[HALO]

        @pl.when(me < n_dev - 1)
        def _():
            halo_copy(slot, src).wait_send()

    lane = lax.broadcasted_iota(jnp.int32, (2, chan), 1)

    def exchange(stage, sums):
        stats[stage, me] = jnp.concatenate([jnp.sum(part, axis=0, keepdims=True) for part in sums], axis=0)

        def copy_to(k):
            return pltpu.make_async_remote_copy(src_ref=stats.at[stage, me], dst_ref=stats.at[stage, me], send_sem=stat_send.at[stage, k], recv_sem=stat_recv.at[stage, n_dev - k], device_id={"time": lax.rem(me + k, n_dev)}, device_id_type=MESH_ID)

        def copy_from(k):
            peer = lax.rem(me + k, n_dev)
            return pltpu.make_async_remote_copy(src_ref=stats.at[stage, peer], dst_ref=stats.at[stage, peer], send_sem=stat_send.at[stage, k], recv_sem=stat_recv.at[stage, k], device_id={"time": peer}, device_id_type=MESH_ID)

        for k in sorted(range(1, n_dev), key=lambda k: abs(2 * k - n_dev)):
            copy_to(k).start()
        for k in range(1, n_dev):
            copy_from(k).wait_recv()
        total = stats[stage, 0]
        for d in range(1, n_dev):
            total = total + stats[stage, d]
        for k in range(1, n_dev):
            copy_to(k).wait_send()
        per_group = chan // GROUPS
        step = 1
        while step < per_group:
            swap = jnp.where(lax.rem(lane, 2 * step) < step, pltpu.roll(total, chan - step, 1), pltpu.roll(total, step, 1))
            total = total + swap
            step *= 2
        mean = total[0:1] / elem_count
        inv_std = lax.rsqrt(total[1:2] / elem_count - mean * mean + NORM_EPS)
        return mean, inv_std * g_ref[pl.ds(stage, 1)], b_ref[pl.ds(stage, 1)]

    def into(ref):
        def emit(frame, i, value, sums):
            ref[HALO + frame, i] = value
            return add_sums(sums, value.astype(F32))
        return emit

    def into_x(frame, i, value, sums):
        value = (x_ref[HALO + frame, i].astype(F32) + value.astype(F32)).astype(BF16)
        x_ref[HALO + frame, i] = value
        return add_sums(sums, value.astype(F32))

    def send_first(slot, src):
        def after(it):
            @pl.when(it == 0)
            def _():
                send_halo(slot, src)
        return after

    zero = jnp.zeros((8, chan), F32)
    sums = (zero, zero)
    for c in reversed(range(CHUNKS)):
        in_copies[c].wait()
        if c == 0:
            for copy in par_copies[-2:]:
                copy.start()

        def add_frame(f, sums):
            return add_sums(sums, x_ref[HALO + c * piece + f].astype(F32))

        sums = lax.fori_loop(0, piece, add_frame, sums)
    with jax.named_scope("barrier"):
        pl.semaphore_wait(barrier, n_dev - 1)
    send_halo(0, x_ref)
    with jax.named_scope("par_wait"):
        for copy in par_copies:
            copy.wait()

    def conv(k, src, emit, after, coef):
        with jax.named_scope("conv"):
            return conv_stage(src, w_ref.at[k], cb_ref[pl.ds(k, 1)], coef, bufs, (zero, zero), emit, after)

    def renorm(stage, sums):
        with jax.named_scope("exchange"):
            return exchange(stage, sums)

    coef = renorm(0, sums)
    take_halo(0, x_ref)
    sums = conv(0, x_ref, into(h_ref), send_first(1, h_ref), coef)
    coef = renorm(1, sums)
    take_halo(1, h_ref)
    sums = conv(1, h_ref, into_x, lambda it: None, coef)
    mean, scale, shift = renorm(2, sums)

    qkv_w = jnp.concatenate([aw_ref[0], aw_ref[1], aw_ref[2]], axis=1)
    qkv_bias = jnp.concatenate([ab_ref[0:1], ab_ref[1:2], ab_ref[2:3]], axis=1)
    out_bias = ab_ref[3:4]
    gain = chan ** -0.5 * 1.4426950408889634
    pairs = ATT // 2

    def attend(it, sums):
        first = HALO + frames - ATT * (it + 1)
        scores, mixed = {}, {}

        def project(p):
            feature = x_ref[pl.ds(first + 2 * p, 2)].astype(F32).reshape(2 * tokens, chan)
            normed = ((feature - mean) * scale + shift).astype(BF16)
            qkv[p % 4] = (dot(normed, qkv_w) + qkv_bias).astype(BF16)

        def score(p):
            for f in range(2):
                mine = slice(f * tokens, (f + 1) * tokens)
                scores[p, f] = lax.dot_general(qkv[p % 4, mine, :chan], qkv[p % 4, mine, chan:2 * chan], (((1,), (1,)), ((), ())), preferred_element_type=F32)

        def softmax(p):
            for f in range(2):
                value = scores.pop((p, f))
                power = jnp.exp2((value - jnp.max(value, axis=1, keepdims=True)) * gain)
                probs[p % 2, f] = (power / jnp.sum(power, axis=1, keepdims=True)).astype(BF16)

        def mix(p):
            for f in range(2):
                mixed[p, f] = dot(probs[p % 2, f], qkv[p % 4, f * tokens:(f + 1) * tokens, 2 * chan:]).astype(BF16)

        def close(p, sums):
            branch = (dot(jnp.concatenate([mixed.pop((p, f)) for f in range(2)], axis=0), aw_ref[3]) + out_bias).astype(BF16)
            value = (x_ref[pl.ds(first + 2 * p, 2)].astype(F32).reshape(2 * tokens, chan) + branch.astype(F32)).astype(BF16)
            h_ref[pl.ds(first + 2 * p, 2)] = value.reshape(2, height, width, chan)
            return add_sums(sums, value.astype(F32))

        for step in range(pairs + 4):
            if 0 <= step - 1 < pairs:
                score(step - 1)
            if 0 <= step - 0 < pairs:
                project(step - 0)
            if 0 <= step - 3 < pairs:
                mix(step - 3)
            if 0 <= step - 2 < pairs:
                softmax(step - 2)
            if 0 <= step - 4 < pairs:
                sums = close(step - 4, sums)

        @pl.when(it == 0)
        def _():
            send_halo(2, h_ref)

        return sums

    with jax.named_scope("attention"):
        sums = lax.fori_loop(0, frames // ATT, attend, (zero, zero))
    coef = renorm(3, sums)
    take_halo(2, h_ref)
    sums = conv(2, h_ref, into(x_ref), send_first(3, x_ref), coef)
    coef = renorm(4, sums)
    take_halo(3, x_ref)
    aux[0:4] = jnp.concatenate([*coef, cb_ref[convs - 1:convs]], axis=0)


def last_kernel(h_ref, x_ref, w_ref, aux, out, y_ref, ua, ub, act_a, act_b, out_sem):
    frames, height, width, chan = y_ref.shape
    clear_act((act_a, act_b), height, width)
    coef = (aux[0:1], aux[1:2], aux[2:3])

    def out_copy(tile):
        span = pl.ds(tile * TILE, TILE)
        return pltpu.make_async_copy(y_ref.at[span], out.at[span], out_sem.at[tile])

    def into_y(frame, i, value, carry):
        y_ref[frame, i] = (x_ref[HALO + frame, i].astype(F32) + value.astype(F32)).astype(BF16)
        return carry

    with jax.named_scope("conv_last"):
        conv_stage(h_ref, w_ref, aux[3:4], coef, (ua, ub, act_a, act_b), 0, into_y, lambda it: None, lambda tile: out_copy(tile).start())
    with jax.named_scope("drain"):
        for tile in range(frames // TILE):
            out_copy(tile).wait()


def solution(mesh):
    n_dev = mesh.shape["time"]
    video_spec = P(("batch", "time"), None, None, None)

    def device_body(latent, conv_w, conv_b, norm_g, norm_b, attn_w, attn_b):
        frames, height, width, chan = latent.shape
        convs = conv_w.shape[0]
        hbm, vmem = pl.BlockSpec(memory_space=pltpu.HBM), pl.BlockSpec(memory_space=pltpu.VMEM)
        padded = (frames + HALO, height, width, chan)
        dma = pltpu.SemaphoreType.DMA
        bufs = [pltpu.VMEM((height, TILE + HALO, width, 3 * chan), BF16)] * 2 + [pltpu.VMEM((TILE + HALO, height * (width + 8) + 8, chan), F32)] * 2
        state = pl.pallas_call(
            functools.partial(kernel, n_dev),
            out_shape=[pltpu.VMEM(padded, BF16), pltpu.VMEM(padded, BF16), pltpu.VMEM(conv_w.shape[1:], BF16), pltpu.VMEM((8, chan), F32)],
            in_specs=[hbm] * 7,
            out_specs=[vmem] * 4,
            scratch_shapes=[
                *bufs,
                pltpu.VMEM((4, 2 * height * width, 3 * chan), BF16),
                pltpu.VMEM((2, 2, height * width, height * width), BF16),
                pltpu.VMEM((convs - 1, *conv_w.shape[1:]), BF16),
                pltpu.VMEM(attn_w.shape, BF16),
                pltpu.VMEM(conv_b.shape, F32),
                pltpu.VMEM(norm_g.shape, F32),
                pltpu.VMEM(norm_b.shape, F32),
                pltpu.VMEM(attn_b.shape, F32),
                pltpu.VMEM((4, HALO, height, width, chan), BF16),
                pltpu.VMEM((5, n_dev, 2, chan), F32),
                dma((CHUNKS,)),
                dma((7,)),
                dma((4,)),
                dma((4,)),
                dma((5, n_dev)),
                dma((5, n_dev)),
            ],
            compiler_params=pltpu.CompilerParams(collective_id=0, has_side_effects=True, vmem_limit_bytes=VMEM_LIMIT),
        )(*(pltpu.with_memory_space_constraint(value, pltpu.HBM) for value in (latent, conv_w, conv_b, norm_g, norm_b, attn_w, attn_b)))
        return pl.pallas_call(
            last_kernel,
            out_shape=jax.ShapeDtypeStruct(latent.shape, latent.dtype),
            in_specs=[vmem] * 4,
            out_specs=hbm,
            scratch_shapes=[pltpu.VMEM(latent.shape, BF16), *bufs, dma((frames // TILE,))],
            compiler_params=pltpu.CompilerParams(vmem_limit_bytes=VMEM_LIMIT),
        )(*state)

    return jax.shard_map(device_body, mesh=mesh, in_specs=(video_spec, P(), P(), P(), P(), P(), P()), out_specs=video_spec, check_vma=False)
```

```python
import functools

import jax
import jax.numpy as jnp
from jax import lax
from jax.experimental import pallas as pl
from jax.experimental.pallas import tpu as pltpu
from jax.sharding import PartitionSpec as P

GROUPS = 32
NORM_EPS = 1e-6
TILE = 8
ATT = 24
CHUNKS = 8
OUT_PIECES = 4
HALO = 2
VMEM_LIMIT = 34 * 2**20
MESH_ID = pl.DeviceIdType.MESH
F32, BF16 = jnp.float32, jnp.bfloat16


def dot(a, b):
    return jnp.dot(a, b, preferred_element_type=F32)


def vreg_sum(value):
    return jnp.sum(value.reshape(-1, 8, value.shape[-1]), axis=0)


def add_sums(sums, value):
    return sums[0] + vreg_sum(value), sums[1] + vreg_sum(value * value)


def norm_tile(src, dst, tile, coef):
    height, width, chan = src.shape[1:]
    mean, scale, shift = coef
    scale, shift = 0.5 * scale, 0.5 * shift
    row = lax.broadcasted_iota(jnp.int32, (8, chan), 0)
    for f in range(TILE + HALO):
        half = (src[tile * TILE + f].astype(F32) - mean) * scale + shift
        value = half + half * jnp.tanh(half)
        dst[:, f, :, chan:2 * chan] = value.astype(BF16)
        for i in range(height):
            gap = jnp.zeros((1, chan), F32)
            left, right = jnp.concatenate([gap, value[i][:width - 1]], axis=0), jnp.concatenate([value[i][1:], gap], axis=0)
            dst[i, f, :, :chan] = left.astype(BF16)
            dst[i, f, :, 2 * chan:] = right.astype(BF16)


def conv_tile(u, w, bias):
    height, _, width, chan = u.shape
    chan //= 3
    zero_w = jnp.zeros((chan, chan), BF16)

    def cols(row, first, count, e):
        return u[row, first:first + count, :, e * chan:(e + 1) * chan].reshape(count * width, chan)

    lhs, rhs = [], []
    for a in range(3):
        for e in range(3):
            for side in range(2):
                lhs.append(jnp.concatenate([cols(g + side, a, TILE, e) for g in range(0, height, 2)], axis=0))
                rhs.append(jnp.concatenate([w[a, 1 + side, e], w[a, side, e]], axis=1))
    main = dot(jnp.concatenate(lhs, axis=1), jnp.concatenate(rhs, axis=0))

    def extra(row, d):
        lhs, rhs = [], []
        for s in range(4):
            for e in range(3):
                lhs.append(jnp.concatenate([cols(row, 2 * p + s, 1, e) for p in range(TILE // 2)], axis=0))
                rhs.append(jnp.concatenate([w[s, d, e] if s < 3 else zero_w, w[s - 1, d, e] if s > 0 else zero_w], axis=1))
        return dot(jnp.concatenate(lhs, axis=1), jnp.concatenate(rhs, axis=0))

    lower = extra(2, 2)
    upper = extra(1, 0)
    rows = []
    for f in range(TILE):
        here = slice(f * width, (f + 1) * width)
        there = slice((TILE + f) * width, (TILE + f + 1) * width)
        pair = slice((f // 2) * width, (f // 2 + 1) * width)
        half = slice((f % 2) * chan, (f % 2 + 1) * chan)
        rows.append([main[here, :chan] + bias, main[here, chan:] + lower[pair, half] + bias, main[there, :chan] + upper[pair, half] + bias, main[there, chan:] + bias])
    return rows


def conv_stage(src, w, bias, coef, bufs, carry, emit, after, done=lambda tile: None):
    ua, ub = bufs
    tiles = (src.shape[0] - HALO) // TILE
    norm_tile(src, ua, tiles - 1, coef)

    def finish(u, tile, carry):
        rows = conv_tile(u, w, bias)
        for f in range(TILE):
            for i in range(len(rows[f])):
                carry = emit(tile * TILE + f, i, rows[f][i].astype(BF16), carry)
        return carry

    def body(it, carry):
        high = tiles - 1 - 2 * it
        norm_tile(src, ub, high - 1, coef)
        carry = finish(ua, high, carry)
        done(high)
        norm_tile(src, ua, jnp.maximum(high - 2, 0), coef)
        carry = finish(ub, high - 1, carry)
        done(high - 1)
        after(it)
        return carry

    return lax.fori_loop(0, tiles // 2, body, carry)


def kernel(n_dev, latent, conv_w, conv_b, norm_g, norm_b, attn_w, attn_b, x_ref, h_ref, w_last, aux, ua, ub, qkv, probs, w_ref, aw_ref, cb_ref, g_ref, b_ref, ab_ref, halo, stats, in_sem, par_sem, halo_send, halo_recv, stat_send, stat_recv):
    frames, height, width, chan = latent.shape
    convs = conv_w.shape[0]
    tokens = height * width
    me = lax.axis_index("time")
    piece = frames // CHUNKS
    elem_count = n_dev * frames * tokens * (chan // GROUPS)
    bufs = (ua, ub)

    in_copies = [pltpu.make_async_copy(latent.at[pl.ds(c * piece, piece)], x_ref.at[pl.ds(HALO + c * piece, piece)], in_sem.at[c]) for c in range(CHUNKS)]
    for c in reversed(range(CHUNKS)):
        in_copies[c].start()
    barrier = pltpu.get_barrier_semaphore()
    for k in range(1, n_dev):
        pl.semaphore_signal(barrier, inc=1, device_id={"time": lax.rem(me + k, n_dev)}, device_id_type=MESH_ID)
    pairs = [(norm_g, g_ref), (norm_b, b_ref), (conv_b, cb_ref), (attn_w, aw_ref), (attn_b, ab_ref), (conv_w.at[pl.ds(0, convs - 1)], w_ref), (conv_w.at[convs - 1], w_last)]
    par_copies = [pltpu.make_async_copy(src, dst, par_sem.at[i]) for i, (src, dst) in enumerate(pairs)]
    for copy in par_copies[:-2]:
        copy.start()

    def halo_copy(slot, src):
        return pltpu.make_async_remote_copy(src_ref=src.at[pl.ds(frames, HALO)], dst_ref=halo.at[slot], send_sem=halo_send.at[slot], recv_sem=halo_recv.at[slot], device_id={"time": lax.rem(me + 1, n_dev)}, device_id_type=MESH_ID)

    def send_halo(slot, src):
        @pl.when(me < n_dev - 1)
        def _():
            halo_copy(slot, src).start()

    def take_halo(slot, src):
        @pl.when(me > 0)
        def _():
            halo_copy(slot, src).wait_recv()
            src[pl.ds(0, HALO)] = halo[slot]

        @pl.when(me == 0)
        def _():
            for f in range(HALO):
                src[f] = src[HALO]

        @pl.when(me < n_dev - 1)
        def _():
            halo_copy(slot, src).wait_send()

    lane = lax.broadcasted_iota(jnp.int32, (2, chan), 1)

    def exchange(stage, sums):
        stats[stage, me] = jnp.concatenate([jnp.sum(part, axis=0, keepdims=True) for part in sums], axis=0)

        def copy_to(k):
            return pltpu.make_async_remote_copy(src_ref=stats.at[stage, me], dst_ref=stats.at[stage, me], send_sem=stat_send.at[stage, k], recv_sem=stat_recv.at[stage, n_dev - k], device_id={"time": lax.rem(me + k, n_dev)}, device_id_type=MESH_ID)

        def copy_from(k):
            peer = lax.rem(me + k, n_dev)
            return pltpu.make_async_remote_copy(src_ref=stats.at[stage, peer], dst_ref=stats.at[stage, peer], send_sem=stat_send.at[stage, k], recv_sem=stat_recv.at[stage, k], device_id={"time": peer}, device_id_type=MESH_ID)

        for k in sorted(range(1, n_dev), key=lambda k: abs(2 * k - n_dev)):
            copy_to(k).start()
        for k in range(1, n_dev):
            copy_from(k).wait_recv()
        total = stats[stage, 0]
        for d in range(1, n_dev):
            total = total + stats[stage, d]
        for k in range(1, n_dev):
            copy_to(k).wait_send()
        per_group = chan // GROUPS
        place, own = lax.rem(lane, per_group), total
        for d in range(1, per_group):
            total = total + jnp.where(place >= d, pltpu.roll(own, d, 1), 0.0) + jnp.where(place < per_group - d, pltpu.roll(own, chan - d, 1), 0.0)
        mean = total[0:1] / elem_count
        inv_std = lax.rsqrt(total[1:2] / elem_count - mean * mean + NORM_EPS)
        return mean, inv_std * g_ref[pl.ds(stage, 1)], b_ref[pl.ds(stage, 1)]

    def into(ref):
        def emit(frame, i, value, sums):
            ref[HALO + frame, i] = value
            return add_sums(sums, value.astype(F32))
        return emit

    def into_x(frame, i, value, sums):
        value = (x_ref[HALO + frame, i].astype(F32) + value.astype(F32)).astype(BF16)
        x_ref[HALO + frame, i] = value
        return add_sums(sums, value.astype(F32))

    def send_first(slot, src):
        def after(it):
            @pl.when(it == 0)
            def _():
                send_halo(slot, src)
        return after

    zero = jnp.zeros((8, chan), F32)
    sums = (zero, zero)
    for c in reversed(range(CHUNKS)):
        in_copies[c].wait()
        if c == 0:
            for copy in par_copies[-2:]:
                copy.start()

        for f in range(piece):
            sums = add_sums(sums, x_ref[HALO + c * piece + f].astype(F32))
    with jax.named_scope("barrier"):
        pl.semaphore_wait(barrier, n_dev - 1)
    send_halo(0, x_ref)
    for copy in par_copies[:-2]:
        copy.wait()

    def conv(k, src, emit, after, coef):
        with jax.named_scope("conv"):
            return conv_stage(src, w_ref.at[k], cb_ref[pl.ds(k, 1)], coef, bufs, (zero, zero), emit, after)

    def renorm(stage, sums):
        with jax.named_scope("exchange"):
            return exchange(stage, sums)

    coef = renorm(0, sums)
    take_halo(0, x_ref)
    for copy in par_copies[-2:]:
        copy.wait()
    sums = conv(0, x_ref, into(h_ref), send_first(1, h_ref), coef)
    coef = renorm(1, sums)
    take_halo(1, h_ref)
    sums = conv(1, h_ref, into_x, lambda it: None, coef)
    mean, scale, shift = renorm(2, sums)

    qkv_w = jnp.concatenate([aw_ref[0], aw_ref[1], aw_ref[2]], axis=1)
    qkv_bias = jnp.concatenate([ab_ref[0:1], ab_ref[1:2], ab_ref[2:3]], axis=1)
    out_bias = ab_ref[3:4]
    gain = chan ** -0.5 * 1.4426950408889634
    pairs = ATT // 2

    def attend(it, sums):
        first = HALO + frames - ATT * (it + 1)
        scores, mixed = {}, {}

        def project(p):
            feature = x_ref[pl.ds(first + 2 * p, 2)].astype(F32).reshape(2 * tokens, chan)
            normed = ((feature - mean) * scale + shift).astype(BF16)
            qkv[p % 4] = (dot(normed, qkv_w) + qkv_bias).astype(BF16)

        def score(p):
            for f in range(2):
                mine = slice(f * tokens, (f + 1) * tokens)
                scores[p, f] = lax.dot_general(qkv[p % 4, mine, :chan], qkv[p % 4, mine, chan:2 * chan], (((1,), (1,)), ((), ())), preferred_element_type=F32)

        def softmax(p):
            for f in range(2):
                value = scores.pop((p, f))
                power = jnp.exp2((value - jnp.max(value, axis=1, keepdims=True)) * gain)
                probs[p % 2, f] = (power / jnp.sum(power, axis=1, keepdims=True)).astype(BF16)

        def mix(p):
            for f in range(2):
                mixed[p, f] = dot(probs[p % 2, f], qkv[p % 4, f * tokens:(f + 1) * tokens, 2 * chan:]).astype(BF16)

        def close(p, sums):
            branch = (dot(jnp.concatenate([mixed.pop((p, f)) for f in range(2)], axis=0), aw_ref[3]) + out_bias).astype(BF16)
            value = (x_ref[pl.ds(first + 2 * p, 2)].astype(F32).reshape(2 * tokens, chan) + branch.astype(F32)).astype(BF16)
            h_ref[pl.ds(first + 2 * p, 2)] = value.reshape(2, height, width, chan)
            return add_sums(sums, value.astype(F32))

        for step in range(pairs + 4):
            if 0 <= step - 0 < pairs:
                project(step - 0)
            if 0 <= step - 1 < pairs:
                score(step - 1)
            if 0 <= step - 2 < pairs:
                softmax(step - 2)
            if 0 <= step - 3 < pairs:
                mix(step - 3)
            if 0 <= step - 4 < pairs:
                sums = close(step - 4, sums)

        @pl.when(it == 0)
        def _():
            send_halo(2, h_ref)

        return sums

    with jax.named_scope("attention"):
        sums = lax.fori_loop(0, frames // ATT, attend, (zero, zero))
    coef = renorm(3, sums)
    take_halo(2, h_ref)
    sums = conv(2, h_ref, into(x_ref), send_first(3, x_ref), coef)
    coef = renorm(4, sums)
    take_halo(3, x_ref)
    aux[0:4] = jnp.concatenate([*coef, cb_ref[convs - 1:convs]], axis=0)


def last_kernel(h_ref, x_ref, w_ref, aux, out, y_ref, ua, ub, out_sem):
    frames, height, width, chan = y_ref.shape
    coef = (aux[0:1], aux[1:2], aux[2:3])

    share = TILE // OUT_PIECES

    def out_copies(tile):
        for n in range(OUT_PIECES):
            span = pl.ds(tile * TILE + n * share, share)
            yield pltpu.make_async_copy(y_ref.at[span], out.at[span], out_sem.at[tile, n])

    def write_out(tile):
        for copy in out_copies(tile):
            copy.start()

    def into_y(frame, i, value, carry):
        y_ref[frame, i] = (x_ref[HALO + frame, i].astype(F32) + value.astype(F32)).astype(BF16)
        return carry

    with jax.named_scope("conv_last"):
        conv_stage(h_ref, w_ref, aux[3:4], coef, (ua, ub), 0, into_y, lambda it: None, write_out)
    with jax.named_scope("drain"):
        for tile in range(frames // TILE):
            for copy in out_copies(tile):
                copy.wait()


def solution(mesh):
    n_dev = mesh.shape["time"]
    video_spec = P(("batch", "time"), None, None, None)

    def device_body(latent, conv_w, conv_b, norm_g, norm_b, attn_w, attn_b):
        frames, height, width, chan = latent.shape
        convs = conv_w.shape[0]
        hbm, vmem = pl.BlockSpec(memory_space=pltpu.HBM), pl.BlockSpec(memory_space=pltpu.VMEM)
        padded = (frames + HALO, height, width, chan)
        dma = pltpu.SemaphoreType.DMA
        bufs = [pltpu.VMEM((height, TILE + HALO, width, 3 * chan), BF16)] * 2
        state = pl.pallas_call(
            functools.partial(kernel, n_dev),
            out_shape=[pltpu.VMEM(padded, BF16), pltpu.VMEM(padded, BF16), pltpu.VMEM(conv_w.shape[1:], BF16), pltpu.VMEM((8, chan), F32)],
            in_specs=[hbm] * 7,
            out_specs=[vmem] * 4,
            scratch_shapes=[
                *bufs,
                pltpu.VMEM((4, 2 * height * width, 3 * chan), BF16),
                pltpu.VMEM((2, 2, height * width, height * width), BF16),
                pltpu.VMEM((convs - 1, *conv_w.shape[1:]), BF16),
                pltpu.VMEM(attn_w.shape, BF16),
                pltpu.VMEM(conv_b.shape, F32),
                pltpu.VMEM(norm_g.shape, F32),
                pltpu.VMEM(norm_b.shape, F32),
                pltpu.VMEM(attn_b.shape, F32),
                pltpu.VMEM((4, HALO, height, width, chan), BF16),
                pltpu.VMEM((5, n_dev, 2, chan), F32),
                dma((CHUNKS,)),
                dma((7,)),
                dma((4,)),
                dma((4,)),
                dma((5, n_dev)),
                dma((5, n_dev)),
            ],
            compiler_params=pltpu.CompilerParams(collective_id=0, has_side_effects=True, vmem_limit_bytes=VMEM_LIMIT),
        )(*(pltpu.with_memory_space_constraint(value, pltpu.HBM) for value in (latent, conv_w, conv_b, norm_g, norm_b, attn_w, attn_b)))
        return pl.pallas_call(
            last_kernel,
            out_shape=jax.ShapeDtypeStruct(latent.shape, latent.dtype),
            in_specs=[vmem] * 4,
            out_specs=hbm,
            scratch_shapes=[pltpu.VMEM(latent.shape, BF16), *bufs, dma((frames // TILE, OUT_PIECES))],
            compiler_params=pltpu.CompilerParams(vmem_limit_bytes=VMEM_LIMIT),
        )(*state)

    return jax.shard_map(device_body, mesh=mesh, in_specs=(video_spec, P(), P(), P(), P(), P(), P()), out_specs=video_spec, check_vma=False)
```

```python
import functools

import jax
import jax.numpy as jnp
from jax import lax
from jax.experimental import pallas as pl
from jax.experimental.pallas import tpu as pltpu
from jax.sharding import PartitionSpec as P

GROUPS = 32
NORM_EPS = 1e-6
TILE = 8
ATT = 24
CHUNKS = 8
OUT_PIECES = 4
HALO = 2
VMEM_LIMIT = 34 * 2**20
MESH_ID = pl.DeviceIdType.MESH
F32, BF16 = jnp.float32, jnp.bfloat16


def dot(a, b):
    return jnp.dot(a, b, preferred_element_type=F32)


def vreg_sum(value):
    return jnp.sum(value.reshape(-1, 8, value.shape[-1]), axis=0)


def add_sums(sums, value):
    return sums[0] + vreg_sum(value), sums[1] + vreg_sum(value * value)


def norm_tile(src, dst, tile, coef):
    height, width, chan = src.shape[1:]
    mean, scale, shift = coef
    scale, shift = 0.5 * scale, 0.5 * shift
    width = src.shape[2]
    first = lax.broadcasted_iota(jnp.int32, (8, chan), 0) == 0
    final = lax.broadcasted_iota(jnp.int32, (8, chan), 0) == 7
    for f in range(TILE + HALO):
        half = (src[tile * TILE + f].astype(F32) - mean) * scale + shift
        value = half + half * jnp.tanh(half)
        dst[:, f, :, chan:2 * chan] = value.astype(BF16)
        for i in range(height):
            wrapped = jnp.where(first, 0.0, pltpu.roll(value[i, width - 8:], 1, 0))
            dst[i, f, :, :chan] = jnp.concatenate([wrapped, value[i, :width - 8]], axis=0).astype(BF16)
            wrapped = jnp.where(final, 0.0, pltpu.roll(value[i, :8], 7, 0))
            dst[i, f, :, 2 * chan:] = jnp.concatenate([value[i, 8:], wrapped], axis=0).astype(BF16)


def conv_tile(u, w, bias):
    height, _, width, chan = u.shape
    chan //= 3
    zero_w = jnp.zeros((chan, chan), BF16)

    def cols(row, first, count, e):
        return u[row, first:first + count, :, e * chan:(e + 1) * chan].reshape(count * width, chan)

    lhs, rhs = [], []
    for a in range(3):
        for e in range(3):
            for side in range(2):
                lhs.append(jnp.concatenate([cols(g + side, a, TILE, e) for g in range(0, height, 2)], axis=0))
                rhs.append(jnp.concatenate([w[a, 1 + side, e], w[a, side, e]], axis=1))
    main = dot(jnp.concatenate(lhs, axis=1), jnp.concatenate(rhs, axis=0))

    def extra(row, d):
        lhs, rhs = [], []
        for s in range(4):
            for e in range(3):
                lhs.append(jnp.concatenate([cols(row, 2 * p + s, 1, e) for p in range(TILE // 2)], axis=0))
                rhs.append(jnp.concatenate([w[s, d, e] if s < 3 else zero_w, w[s - 1, d, e] if s > 0 else zero_w], axis=1))
        return dot(jnp.concatenate(lhs, axis=1), jnp.concatenate(rhs, axis=0))

    lower = extra(2, 2)
    upper = extra(1, 0)
    rows = []
    for f in range(TILE):
        here = slice(f * width, (f + 1) * width)
        there = slice((TILE + f) * width, (TILE + f + 1) * width)
        pair = slice((f // 2) * width, (f // 2 + 1) * width)
        half = slice((f % 2) * chan, (f % 2 + 1) * chan)
        rows.append([main[here, :chan] + bias, main[here, chan:] + lower[pair, half] + bias, main[there, :chan] + upper[pair, half] + bias, main[there, chan:] + bias])
    return rows


def conv_stage(src, w, bias, coef, bufs, carry, emit, after, done=lambda tile: None):
    ua, ub = bufs
    tiles = (src.shape[0] - HALO) // TILE
    norm_tile(src, ua, tiles - 1, coef)

    def finish(u, tile, carry):
        rows = conv_tile(u, w, bias)
        for f in range(TILE):
            for i in range(len(rows[f])):
                carry = emit(tile * TILE + f, i, rows[f][i].astype(BF16), carry)
        return carry

    def body(it, carry):
        high = tiles - 1 - 2 * it
        norm_tile(src, ub, high - 1, coef)
        carry = finish(ua, high, carry)
        done(high)
        norm_tile(src, ua, jnp.maximum(high - 2, 0), coef)
        carry = finish(ub, high - 1, carry)
        done(high - 1)
        after(it)
        return carry

    return lax.fori_loop(0, tiles // 2, body, carry)


def kernel(n_dev, latent, conv_w, conv_b, norm_g, norm_b, attn_w, attn_b, x_ref, h_ref, w_last, aux, raw, flat, ua, ub, qkv, probs, w_ref, aw_ref, cb_ref, g_ref, b_ref, ab_ref, halo, stats, in_sem, par_sem, halo_send, halo_recv, stat_send, stat_recv):
    frames, height, width, chan = latent.shape
    convs = conv_w.shape[0]
    tokens = height * width
    me = lax.axis_index("time")
    piece = frames // CHUNKS
    elem_count = n_dev * frames * tokens * (chan // GROUPS)
    bufs = (ua, ub)

    in_copies = [pltpu.make_async_copy(latent.at[pl.ds(c * piece, piece)], raw.at[pl.ds(c * piece, piece)], in_sem.at[c]) for c in range(CHUNKS)]
    for c in reversed(range(CHUNKS)):
        in_copies[c].start()
    barrier = pltpu.get_barrier_semaphore()
    for k in range(1, n_dev):
        pl.semaphore_signal(barrier, inc=1, device_id={"time": lax.rem(me + k, n_dev)}, device_id_type=MESH_ID)
    pairs = [(norm_g, g_ref), (norm_b, b_ref), (conv_b, cb_ref), (attn_w, aw_ref), (attn_b, ab_ref), (conv_w.at[pl.ds(0, convs - 1)], w_ref), (conv_w.at[convs - 1], w_last)]
    par_copies = [pltpu.make_async_copy(src, dst, par_sem.at[i]) for i, (src, dst) in enumerate(pairs)]
    for copy in par_copies[:-2]:
        copy.start()

    def halo_copy(slot, src):
        return pltpu.make_async_remote_copy(src_ref=src.at[pl.ds(frames, HALO)], dst_ref=halo.at[slot], send_sem=halo_send.at[slot], recv_sem=halo_recv.at[slot], device_id={"time": lax.rem(me + 1, n_dev)}, device_id_type=MESH_ID)

    def send_halo(slot, src):
        @pl.when(me < n_dev - 1)
        def _():
            halo_copy(slot, src).start()

    def take_halo(slot, src):
        @pl.when(me > 0)
        def _():
            halo_copy(slot, src).wait_recv()
            src[pl.ds(0, HALO)] = halo[slot]

        @pl.when(me == 0)
        def _():
            for f in range(HALO):
                src[f] = src[HALO]

        @pl.when(me < n_dev - 1)
        def _():
            halo_copy(slot, src).wait_send()

    lane = lax.broadcasted_iota(jnp.int32, (2, chan), 1)

    def exchange(stage, sums):
        stats[stage, me] = jnp.concatenate([jnp.sum(part, axis=0, keepdims=True) for part in sums], axis=0)

        def copy_to(k):
            return pltpu.make_async_remote_copy(src_ref=stats.at[stage, me], dst_ref=stats.at[stage, me], send_sem=stat_send.at[stage, k], recv_sem=stat_recv.at[stage, n_dev - k], device_id={"time": lax.rem(me + k, n_dev)}, device_id_type=MESH_ID)

        def copy_from(k):
            peer = lax.rem(me + k, n_dev)
            return pltpu.make_async_remote_copy(src_ref=stats.at[stage, peer], dst_ref=stats.at[stage, peer], send_sem=stat_send.at[stage, k], recv_sem=stat_recv.at[stage, k], device_id={"time": peer}, device_id_type=MESH_ID)

        for k in sorted(range(1, n_dev), key=lambda k: abs(2 * k - n_dev)):
            copy_to(k).start()
        for k in range(1, n_dev):
            copy_from(k).wait_recv()
        total = stats[stage, 0]
        for d in range(1, n_dev):
            total = total + stats[stage, d]
        for k in range(1, n_dev):
            copy_to(k).wait_send()
        per_group = chan // GROUPS
        place, own = lax.rem(lane, per_group), total
        for d in range(1, per_group):
            total = total + jnp.where(place >= d, pltpu.roll(own, d, 1), 0.0) + jnp.where(place < per_group - d, pltpu.roll(own, chan - d, 1), 0.0)
        mean = total[0:1] / elem_count
        inv_std = lax.rsqrt(total[1:2] / elem_count - mean * mean + NORM_EPS)
        return mean, inv_std * g_ref[pl.ds(stage, 1)], b_ref[pl.ds(stage, 1)]

    def into(ref):
        def emit(frame, i, value, sums):
            ref[HALO + frame, i] = value
            return add_sums(sums, value.astype(F32))
        return emit

    def into_x(frame, i, value, sums):
        value = (x_ref[HALO + frame, i].astype(F32) + value.astype(F32)).astype(BF16)
        x_ref[HALO + frame, i] = value
        return add_sums(sums, value.astype(F32))

    def send_first(slot, src):
        def after(it):
            @pl.when(it == 0)
            def _():
                send_halo(slot, src)
        return after

    zero = jnp.zeros((8, chan), F32)
    sums = (zero, zero)
    for c in reversed(range(CHUNKS)):
        in_copies[c].wait()
        if c == 0:
            for copy in par_copies[-2:]:
                copy.start()

        for f in range(piece):
            value = raw[c * piece + f].astype(F32)
            sums = add_sums(sums, value)
            flat[f] = value
            value = jnp.concatenate([flat[f, :, pl.ds(v, 8, stride=width // 8)] for v in range(width // 8)], axis=1)
            x_ref[HALO + c * piece + f] = value.astype(BF16)
    with jax.named_scope("barrier"):
        pl.semaphore_wait(barrier, n_dev - 1)
    send_halo(0, x_ref)
    for copy in par_copies[:-2]:
        copy.wait()

    def conv(k, src, emit, after, coef):
        with jax.named_scope("conv"):
            return conv_stage(src, w_ref.at[k], cb_ref[pl.ds(k, 1)], coef, bufs, (zero, zero), emit, after)

    def renorm(stage, sums):
        with jax.named_scope("exchange"):
            return exchange(stage, sums)

    coef = renorm(0, sums)
    take_halo(0, x_ref)
    for copy in par_copies[-2:]:
        copy.wait()
    sums = conv(0, x_ref, into(h_ref), send_first(1, h_ref), coef)
    coef = renorm(1, sums)
    take_halo(1, h_ref)
    sums = conv(1, h_ref, into_x, lambda it: None, coef)
    mean, scale, shift = renorm(2, sums)

    qkv_w = jnp.concatenate([aw_ref[0], aw_ref[1], aw_ref[2]], axis=1)
    qkv_bias = jnp.concatenate([ab_ref[0:1], ab_ref[1:2], ab_ref[2:3]], axis=1)
    out_bias = ab_ref[3:4]
    gain = chan ** -0.5 * 1.4426950408889634
    pairs = ATT // 2

    def attend(it, sums):
        first = HALO + frames - ATT * (it + 1)
        scores, mixed = {}, {}

        def project(p):
            feature = x_ref[pl.ds(first + 2 * p, 2)].astype(F32).reshape(2 * tokens, chan)
            normed = ((feature - mean) * scale + shift).astype(BF16)
            qkv[p % 4] = (dot(normed, qkv_w) + qkv_bias).astype(BF16)

        def score(p):
            for f in range(2):
                mine = slice(f * tokens, (f + 1) * tokens)
                scores[p, f] = lax.dot_general(qkv[p % 4, mine, :chan], qkv[p % 4, mine, chan:2 * chan], (((1,), (1,)), ((), ())), preferred_element_type=F32)

        def softmax(p):
            for f in range(2):
                value = scores.pop((p, f))
                power = jnp.exp2((value - jnp.max(value, axis=1, keepdims=True)) * gain)
                probs[p % 2, f] = (power / jnp.sum(power, axis=1, keepdims=True)).astype(BF16)

        def mix(p):
            for f in range(2):
                mixed[p, f] = dot(probs[p % 2, f], qkv[p % 4, f * tokens:(f + 1) * tokens, 2 * chan:]).astype(BF16)

        def close(p, sums):
            branch = (dot(jnp.concatenate([mixed.pop((p, f)) for f in range(2)], axis=0), aw_ref[3]) + out_bias).astype(BF16)
            value = (x_ref[pl.ds(first + 2 * p, 2)].astype(F32).reshape(2 * tokens, chan) + branch.astype(F32)).astype(BF16)
            h_ref[pl.ds(first + 2 * p, 2)] = value.reshape(2, height, width, chan)
            return add_sums(sums, value.astype(F32))

        for step in range(pairs + 4):
            if 0 <= step - 0 < pairs:
                project(step - 0)
            if 0 <= step - 1 < pairs:
                score(step - 1)
            if 0 <= step - 2 < pairs:
                softmax(step - 2)
            if 0 <= step - 3 < pairs:
                mix(step - 3)
            if 0 <= step - 4 < pairs:
                sums = close(step - 4, sums)

        @pl.when(it == 0)
        def _():
            send_halo(2, h_ref)

        return sums

    with jax.named_scope("attention"):
        sums = lax.fori_loop(0, frames // ATT, attend, (zero, zero))
    coef = renorm(3, sums)
    take_halo(2, h_ref)
    sums = conv(2, h_ref, into(x_ref), send_first(3, x_ref), coef)
    coef = renorm(4, sums)
    take_halo(3, x_ref)
    aux[0:4] = jnp.concatenate([*coef, cb_ref[convs - 1:convs]], axis=0)


def last_kernel(h_ref, x_ref, w_ref, aux, out, y_ref, flat, ua, ub, out_sem):
    frames, height, width, chan = y_ref.shape
    coef = (aux[0:1], aux[1:2], aux[2:3])

    share = TILE // OUT_PIECES

    def out_copies(tile):
        for n in range(OUT_PIECES):
            span = pl.ds(tile * TILE + n * share, share)
            yield pltpu.make_async_copy(y_ref.at[span], out.at[span], out_sem.at[tile, n])

    def write_out(tile):
        for copy in out_copies(tile):
            copy.start()

    def into_y(frame, i, value, carry):
        value = (x_ref[HALO + frame, i].astype(F32) + value.astype(F32)).astype(BF16).astype(F32)
        slot = i % 2
        for v in range(width // 8):
            flat[slot, pl.ds(v, 8, stride=width // 8)] = value[8 * v:8 * v + 8]
        y_ref[frame, i] = flat[slot].astype(BF16)
        return carry

    with jax.named_scope("conv_last"):
        conv_stage(h_ref, w_ref, aux[3:4], coef, (ua, ub), 0, into_y, lambda it: None, write_out)
    with jax.named_scope("drain"):
        for tile in range(frames // TILE):
            for copy in out_copies(tile):
                copy.wait()


def solution(mesh):
    n_dev = mesh.shape["time"]
    video_spec = P(("batch", "time"), None, None, None)

    def device_body(latent, conv_w, conv_b, norm_g, norm_b, attn_w, attn_b):
        frames, height, width, chan = latent.shape
        convs = conv_w.shape[0]
        hbm, vmem = pl.BlockSpec(memory_space=pltpu.HBM), pl.BlockSpec(memory_space=pltpu.VMEM)
        padded = (frames + HALO, height, width, chan)
        dma = pltpu.SemaphoreType.DMA
        bufs = [pltpu.VMEM((height, TILE + HALO, width, 3 * chan), BF16)] * 2
        state = pl.pallas_call(
            functools.partial(kernel, n_dev),
            out_shape=[pltpu.VMEM(padded, BF16), pltpu.VMEM(padded, BF16), pltpu.VMEM(conv_w.shape[1:], BF16), pltpu.VMEM((8, chan), F32)],
            in_specs=[hbm] * 7,
            out_specs=[vmem] * 4,
            scratch_shapes=[
                pltpu.VMEM(latent.shape, BF16),
                pltpu.VMEM((frames // CHUNKS, height, width, chan), F32),
                *bufs,
                pltpu.VMEM((4, 2 * height * width, 3 * chan), BF16),
                pltpu.VMEM((2, 2, height * width, height * width), BF16),
                pltpu.VMEM((convs - 1, *conv_w.shape[1:]), BF16),
                pltpu.VMEM(attn_w.shape, BF16),
                pltpu.VMEM(conv_b.shape, F32),
                pltpu.VMEM(norm_g.shape, F32),
                pltpu.VMEM(norm_b.shape, F32),
                pltpu.VMEM(attn_b.shape, F32),
                pltpu.VMEM((4, HALO, height, width, chan), BF16),
                pltpu.VMEM((5, n_dev, 2, chan), F32),
                dma((CHUNKS,)),
                dma((7,)),
                dma((4,)),
                dma((4,)),
                dma((5, n_dev)),
                dma((5, n_dev)),
            ],
            compiler_params=pltpu.CompilerParams(collective_id=0, has_side_effects=True, vmem_limit_bytes=VMEM_LIMIT),
        )(*(pltpu.with_memory_space_constraint(value, pltpu.HBM) for value in (latent, conv_w, conv_b, norm_g, norm_b, attn_w, attn_b)))
        return pl.pallas_call(
            last_kernel,
            out_shape=jax.ShapeDtypeStruct(latent.shape, latent.dtype),
            in_specs=[vmem] * 4,
            out_specs=hbm,
            scratch_shapes=[pltpu.VMEM(latent.shape, BF16), pltpu.VMEM((2, width, chan), F32), *bufs, dma((frames // TILE, OUT_PIECES))],
            compiler_params=pltpu.CompilerParams(vmem_limit_bytes=VMEM_LIMIT),
        )(*state)

    return jax.shard_map(device_body, mesh=mesh, in_specs=(video_spec, P(), P(), P(), P(), P(), P()), out_specs=video_spec, check_vma=False)
```

```python
import functools

import jax
import jax.numpy as jnp
from jax import lax
from jax.experimental import pallas as pl
from jax.experimental.pallas import tpu as pltpu
from jax.sharding import PartitionSpec as P

GROUPS = 32
NORM_EPS = 1e-6
TILE = 8
ATT = 24
CHUNKS = 8
OUT_PIECES = 4
HALO = 2
VMEM_LIMIT = 34 * 2**20
MESH_ID = pl.DeviceIdType.MESH
F32, BF16 = jnp.float32, jnp.bfloat16


def dot(a, b):
    return jnp.dot(a, b, preferred_element_type=F32)


def vreg_sum(value):
    return jnp.sum(value.reshape(-1, 8, value.shape[-1]), axis=0)


def add_sums(sums, value):
    return sums[0] + vreg_sum(value), sums[1] + vreg_sum(value * value)


def norm_tile(src, dst, tile, coef):
    height, width, chan = src.shape[1:]
    mean, scale, shift = coef
    scale, shift = 0.5 * scale, 0.5 * shift
    width = src.shape[2]
    first = lax.broadcasted_iota(jnp.int32, (8, chan), 0) == 0
    final = lax.broadcasted_iota(jnp.int32, (8, chan), 0) == 7
    for f in range(TILE + HALO):
        half = (src[tile * TILE + f].astype(F32) - mean) * scale + shift
        value = half + half * jnp.tanh(half)
        dst[:, f, :, chan:2 * chan] = value.astype(BF16)
        for i in range(height):
            wrapped = jnp.where(first, 0.0, pltpu.roll(value[i, width - 8:], 1, 0))
            dst[i, f, :, :chan] = jnp.concatenate([wrapped, value[i, :width - 8]], axis=0).astype(BF16)
            wrapped = jnp.where(final, 0.0, pltpu.roll(value[i, :8], 7, 0))
            dst[i, f, :, 2 * chan:] = jnp.concatenate([value[i, 8:], wrapped], axis=0).astype(BF16)


def conv_tile(u, w, bias):
    height, _, width, chan = u.shape
    chan //= 3
    zero_w = jnp.zeros((chan, chan), BF16)

    def cols(row, first, count, e):
        return u[row, first:first + count, :, e * chan:(e + 1) * chan].reshape(count * width, chan)

    lhs, rhs = [], []
    for a in range(3):
        for e in range(3):
            for side in range(2):
                lhs.append(jnp.concatenate([cols(g + side, a, TILE, e) for g in range(0, height, 2)], axis=0))
                rhs.append(jnp.concatenate([w[a, 1 + side, e], w[a, side, e]], axis=1))
    main = dot(jnp.concatenate(lhs, axis=1), jnp.concatenate(rhs, axis=0))

    def extra(row, d):
        lhs, rhs = [], []
        for s in range(4):
            for e in range(3):
                lhs.append(jnp.concatenate([cols(row, 2 * p + s, 1, e) for p in range(TILE // 2)], axis=0))
                rhs.append(jnp.concatenate([w[s, d, e] if s < 3 else zero_w, w[s - 1, d, e] if s > 0 else zero_w], axis=1))
        return dot(jnp.concatenate(lhs, axis=1), jnp.concatenate(rhs, axis=0))

    lower = extra(2, 2)
    upper = extra(1, 0)
    rows = []
    for f in range(TILE):
        here = slice(f * width, (f + 1) * width)
        there = slice((TILE + f) * width, (TILE + f + 1) * width)
        pair = slice((f // 2) * width, (f // 2 + 1) * width)
        half = slice((f % 2) * chan, (f % 2 + 1) * chan)
        rows.append([main[here, :chan] + bias, main[here, chan:] + lower[pair, half] + bias, main[there, :chan] + upper[pair, half] + bias, main[there, chan:] + bias])
    return rows


def conv_stage(src, w, bias, coef, bufs, carry, emit, after, done=lambda tile: None):
    ua, ub = bufs
    tiles = (src.shape[0] - HALO) // TILE
    norm_tile(src, ua, tiles - 1, coef)

    def finish(u, tile, carry):
        rows = conv_tile(u, w, bias)
        for f in range(TILE):
            for i in range(len(rows[f])):
                carry = emit(tile * TILE + f, i, rows[f][i].astype(BF16), carry)
        return carry

    def body(it, carry):
        high = tiles - 1 - 2 * it
        norm_tile(src, ub, high - 1, coef)
        carry = finish(ua, high, carry)
        done(high)
        norm_tile(src, ua, jnp.maximum(high - 2, 0), coef)
        carry = finish(ub, high - 1, carry)
        done(high - 1)
        after(it)
        return carry

    return lax.fori_loop(0, tiles // 2, body, carry)


def kernel(n_dev, latent, conv_w, conv_b, norm_g, norm_b, attn_w, attn_b, x_ref, h_ref, w_last, aux, raw, flat, ua, ub, qkv, probs, w_ref, aw_ref, cb_ref, g_ref, b_ref, ab_ref, halo, stats, in_sem, par_sem, halo_send, halo_recv, stat_send, stat_recv):
    frames, height, width, chan = latent.shape
    convs = conv_w.shape[0]
    tokens = height * width
    me = lax.axis_index("time")
    piece = frames // CHUNKS
    elem_count = n_dev * frames * tokens * (chan // GROUPS)
    bufs = (ua, ub)

    in_copies = [pltpu.make_async_copy(latent.at[pl.ds(c * piece, piece)], raw.at[pl.ds(c * piece, piece)], in_sem.at[c]) for c in range(CHUNKS)]
    for c in reversed(range(CHUNKS)):
        in_copies[c].start()
    barrier = pltpu.get_barrier_semaphore()
    for k in range(1, n_dev):
        pl.semaphore_signal(barrier, inc=1, device_id={"time": lax.rem(me + k, n_dev)}, device_id_type=MESH_ID)
    pairs = [(norm_g, g_ref), (norm_b, b_ref), (conv_b, cb_ref), (attn_w, aw_ref), (attn_b, ab_ref), (conv_w.at[pl.ds(0, convs - 1)], w_ref), (conv_w.at[convs - 1], w_last)]
    par_copies = [pltpu.make_async_copy(src, dst, par_sem.at[i]) for i, (src, dst) in enumerate(pairs)]
    for copy in par_copies[:-2]:
        copy.start()

    def halo_copy(slot, src):
        return pltpu.make_async_remote_copy(src_ref=src.at[pl.ds(frames, HALO)], dst_ref=halo.at[slot], send_sem=halo_send.at[slot], recv_sem=halo_recv.at[slot], device_id={"time": lax.rem(me + 1, n_dev)}, device_id_type=MESH_ID)

    def send_halo(slot, src):
        @pl.when(me < n_dev - 1)
        def _():
            halo_copy(slot, src).start()

    def take_halo(slot, src):
        @pl.when(me > 0)
        def _():
            halo_copy(slot, src).wait_recv()
            src[pl.ds(0, HALO)] = halo[slot]

        @pl.when(me == 0)
        def _():
            for f in range(HALO):
                src[f] = src[HALO]

        @pl.when(me < n_dev - 1)
        def _():
            halo_copy(slot, src).wait_send()

    lane = lax.broadcasted_iota(jnp.int32, (2, chan), 1)

    def exchange(stage, sums, meanwhile):
        stats[stage, me] = jnp.concatenate([jnp.sum(part, axis=0, keepdims=True) for part in sums], axis=0)

        def copy_to(k):
            return pltpu.make_async_remote_copy(src_ref=stats.at[stage, me], dst_ref=stats.at[stage, me], send_sem=stat_send.at[stage, k], recv_sem=stat_recv.at[stage, n_dev - k], device_id={"time": lax.rem(me + k, n_dev)}, device_id_type=MESH_ID)

        def copy_from(k):
            peer = lax.rem(me + k, n_dev)
            return pltpu.make_async_remote_copy(src_ref=stats.at[stage, peer], dst_ref=stats.at[stage, peer], send_sem=stat_send.at[stage, k], recv_sem=stat_recv.at[stage, k], device_id={"time": peer}, device_id_type=MESH_ID)

        for k in sorted(range(1, n_dev), key=lambda k: abs(2 * k - n_dev)):
            copy_to(k).start()
        meanwhile()
        for k in range(1, n_dev):
            copy_from(k).wait_recv()
        total = stats[stage, 0]
        for d in range(1, n_dev):
            total = total + stats[stage, d]
        for k in range(1, n_dev):
            copy_to(k).wait_send()
        per_group = chan // GROUPS
        place, own = lax.rem(lane, per_group), total
        for d in range(1, per_group):
            total = total + jnp.where(place >= d, pltpu.roll(own, d, 1), 0.0) + jnp.where(place < per_group - d, pltpu.roll(own, chan - d, 1), 0.0)
        mean = total[0:1] / elem_count
        inv_std = lax.rsqrt(total[1:2] / elem_count - mean * mean + NORM_EPS)
        return mean, inv_std * g_ref[pl.ds(stage, 1)], b_ref[pl.ds(stage, 1)]

    def into(ref):
        def emit(frame, i, value, sums):
            ref[HALO + frame, i] = value
            return add_sums(sums, value.astype(F32))
        return emit

    def into_x(frame, i, value, sums):
        value = (x_ref[HALO + frame, i].astype(F32) + value.astype(F32)).astype(BF16)
        x_ref[HALO + frame, i] = value
        return add_sums(sums, value.astype(F32))

    def send_first(slot, src):
        def after(it):
            @pl.when(it == 0)
            def _():
                send_halo(slot, src)
        return after

    zero = jnp.zeros((8, chan), F32)
    sums = (zero, zero)
    for c in reversed(range(CHUNKS)):
        in_copies[c].wait()
        if c == 0:
            for copy in par_copies[-2:]:
                copy.start()

        for f in range(piece):
            sums = add_sums(sums, raw[c * piece + f].astype(F32))
    with jax.named_scope("barrier"):
        pl.semaphore_wait(barrier, n_dev - 1)

    def reorder(n):
        start = frames - piece * (n + 1)
        for f in range(piece):
            flat[f] = raw[start + f].astype(F32)
            value = jnp.concatenate([flat[f, :, pl.ds(v, 8, stride=width // 8)] for v in range(width // 8)], axis=1)
            x_ref[HALO + start + f] = value.astype(BF16)

    def while_sums_travel():
        reorder(0)
        reorder(1)
        send_halo(0, x_ref)
        for n in range(2, CHUNKS):
            reorder(n)
        for copy in par_copies:
            copy.wait()
        take_halo(0, x_ref)

    def conv(k, src, emit, after, coef):
        with jax.named_scope("conv"):
            return conv_stage(src, w_ref.at[k], cb_ref[pl.ds(k, 1)], coef, bufs, (zero, zero), emit, after)

    def renorm(stage, sums, meanwhile=lambda: None):
        with jax.named_scope("exchange"):
            return exchange(stage, sums, meanwhile)

    coef = renorm(0, sums, while_sums_travel)
    sums = conv(0, x_ref, into(h_ref), send_first(1, h_ref), coef)
    coef = renorm(1, sums, lambda: take_halo(1, h_ref))
    sums = conv(1, h_ref, into_x, lambda it: None, coef)
    mean, scale, shift = renorm(2, sums)

    qkv_w = jnp.concatenate([aw_ref[0], aw_ref[1], aw_ref[2]], axis=1)
    qkv_bias = jnp.concatenate([ab_ref[0:1], ab_ref[1:2], ab_ref[2:3]], axis=1)
    out_bias = ab_ref[3:4]
    gain = chan ** -0.5 * 1.4426950408889634
    pairs = ATT // 2

    def attend(it, sums):
        first = HALO + frames - ATT * (it + 1)
        scores, mixed = {}, {}

        def project(p):
            feature = x_ref[pl.ds(first + 2 * p, 2)].astype(F32).reshape(2 * tokens, chan)
            normed = ((feature - mean) * scale + shift).astype(BF16)
            qkv[p % 4] = (dot(normed, qkv_w) + qkv_bias).astype(BF16)

        def score(p):
            for f in range(2):
                mine = slice(f * tokens, (f + 1) * tokens)
                scores[p, f] = lax.dot_general(qkv[p % 4, mine, :chan], qkv[p % 4, mine, chan:2 * chan], (((1,), (1,)), ((), ())), preferred_element_type=F32)

        def softmax(p):
            for f in range(2):
                value = scores.pop((p, f))
                power = jnp.exp2((value - jnp.max(value, axis=1, keepdims=True)) * gain)
                probs[p % 2, f] = (power / jnp.sum(power, axis=1, keepdims=True)).astype(BF16)

        def mix(p):
            for f in range(2):
                mixed[p, f] = dot(probs[p % 2, f], qkv[p % 4, f * tokens:(f + 1) * tokens, 2 * chan:]).astype(BF16)

        def close(p, sums):
            branch = (dot(jnp.concatenate([mixed.pop((p, f)) for f in range(2)], axis=0), aw_ref[3]) + out_bias).astype(BF16)
            value = (x_ref[pl.ds(first + 2 * p, 2)].astype(F32).reshape(2 * tokens, chan) + branch.astype(F32)).astype(BF16)
            h_ref[pl.ds(first + 2 * p, 2)] = value.reshape(2, height, width, chan)
            return add_sums(sums, value.astype(F32))

        for step in range(pairs + 4):
            if 0 <= step - 0 < pairs:
                project(step - 0)
            if 0 <= step - 1 < pairs:
                score(step - 1)
            if 0 <= step - 2 < pairs:
                softmax(step - 2)
            if 0 <= step - 3 < pairs:
                mix(step - 3)
            if 0 <= step - 4 < pairs:
                sums = close(step - 4, sums)

        @pl.when(it == 0)
        def _():
            send_halo(2, h_ref)

        return sums

    with jax.named_scope("attention"):
        sums = lax.fori_loop(0, frames // ATT, attend, (zero, zero))
    coef = renorm(3, sums, lambda: take_halo(2, h_ref))
    sums = conv(2, h_ref, into(x_ref), send_first(3, x_ref), coef)
    coef = renorm(4, sums, lambda: take_halo(3, x_ref))
    aux[0:4] = jnp.concatenate([*coef, cb_ref[convs - 1:convs]], axis=0)


def last_kernel(h_ref, x_ref, w_ref, aux, out, y_ref, flat, ua, ub, out_sem):
    frames, height, width, chan = y_ref.shape
    coef = (aux[0:1], aux[1:2], aux[2:3])

    share = TILE // OUT_PIECES

    def out_copies(tile):
        for n in range(OUT_PIECES):
            span = pl.ds(tile * TILE + n * share, share)
            yield pltpu.make_async_copy(y_ref.at[span], out.at[span], out_sem.at[tile, n])

    def write_out(tile):
        for copy in out_copies(tile):
            copy.start()

    def into_y(frame, i, value, carry):
        value = (x_ref[HALO + frame, i].astype(F32) + value.astype(F32)).astype(BF16).astype(F32)
        slot = i % 2
        for v in range(width // 8):
            flat[slot, pl.ds(v, 8, stride=width // 8)] = value[8 * v:8 * v + 8]
        y_ref[frame, i] = flat[slot].astype(BF16)
        return carry

    with jax.named_scope("conv_last"):
        conv_stage(h_ref, w_ref, aux[3:4], coef, (ua, ub), 0, into_y, lambda it: None, write_out)
    with jax.named_scope("drain"):
        for tile in range(frames // TILE):
            for copy in out_copies(tile):
                copy.wait()


def solution(mesh):
    n_dev = mesh.shape["time"]
    video_spec = P(("batch", "time"), None, None, None)

    def device_body(latent, conv_w, conv_b, norm_g, norm_b, attn_w, attn_b):
        frames, height, width, chan = latent.shape
        convs = conv_w.shape[0]
        hbm, vmem = pl.BlockSpec(memory_space=pltpu.HBM), pl.BlockSpec(memory_space=pltpu.VMEM)
        padded = (frames + HALO, height, width, chan)
        dma = pltpu.SemaphoreType.DMA
        bufs = [pltpu.VMEM((height, TILE + HALO, width, 3 * chan), BF16)] * 2
        state = pl.pallas_call(
            functools.partial(kernel, n_dev),
            out_shape=[pltpu.VMEM(padded, BF16), pltpu.VMEM(padded, BF16), pltpu.VMEM(conv_w.shape[1:], BF16), pltpu.VMEM((8, chan), F32)],
            in_specs=[hbm] * 7,
            out_specs=[vmem] * 4,
            scratch_shapes=[
                pltpu.VMEM(latent.shape, BF16),
                pltpu.VMEM((frames // CHUNKS, height, width, chan), F32),
                *bufs,
                pltpu.VMEM((4, 2 * height * width, 3 * chan), BF16),
                pltpu.VMEM((2, 2, height * width, height * width), BF16),
                pltpu.VMEM((convs - 1, *conv_w.shape[1:]), BF16),
                pltpu.VMEM(attn_w.shape, BF16),
                pltpu.VMEM(conv_b.shape, F32),
                pltpu.VMEM(norm_g.shape, F32),
                pltpu.VMEM(norm_b.shape, F32),
                pltpu.VMEM(attn_b.shape, F32),
                pltpu.VMEM((4, HALO, height, width, chan), BF16),
                pltpu.VMEM((5, n_dev, 2, chan), F32),
                dma((CHUNKS,)),
                dma((7,)),
                dma((4,)),
                dma((4,)),
                dma((5, n_dev)),
                dma((5, n_dev)),
            ],
            compiler_params=pltpu.CompilerParams(collective_id=0, has_side_effects=True, vmem_limit_bytes=VMEM_LIMIT),
        )(*(pltpu.with_memory_space_constraint(value, pltpu.HBM) for value in (latent, conv_w, conv_b, norm_g, norm_b, attn_w, attn_b)))
        return pl.pallas_call(
            last_kernel,
            out_shape=jax.ShapeDtypeStruct(latent.shape, latent.dtype),
            in_specs=[vmem] * 4,
            out_specs=hbm,
            scratch_shapes=[pltpu.VMEM(latent.shape, BF16), pltpu.VMEM((2, width, chan), F32), *bufs, dma((frames // TILE, OUT_PIECES))],
            compiler_params=pltpu.CompilerParams(vmem_limit_bytes=VMEM_LIMIT),
        )(*state)

    return jax.shard_map(device_body, mesh=mesh, in_specs=(video_spec, P(), P(), P(), P(), P(), P()), out_specs=video_spec, check_vma=False)
```
